128 devices in a mesh: dp: 128 (over z, y, x, core).
Axes of the slice: x: 4, y: 4, z: 4, core: 2. Of those that a mesh axis runs over, the one named last changes fastest.
Arguments:
- x_layer0: bfloat16 [128, 1024, 576], P('dp')
- x_layer1: bfloat16 [128, 1024, 576], P('dp')
- d_out: bfloat16 [128, 1024, 576], P('dp')
- g_attn: bfloat16 [2, 576], replicated
- w_q: bfloat16 [2, 576, 9, 64], replicated
- w_k: bfloat16 [2, 576, 3, 64], replicated
- w_v: bfloat16 [2, 576, 3, 64], replicated
- w_o: bfloat16 [2, 9, 64, 576], replicated
- g_ffn: bfloat16 [2, 576], replicated
- w_gate: bfloat16 [2, 576, 1536], replicated
- w_up: bfloat16 [2, 576, 1536], replicated
- w_down: bfloat16 [2, 1536, 576], replicated
Outputs:
- output 1: bfloat16 [128, 1024, 576], P('dp')
- output 2: float32 [2, 576], replicated
- output 3: float32 [2, 576, 9, 64], replicated
- output 4: float32 [2, 576, 3, 64], replicated
- output 5: float32 [2, 576, 3, 64], replicated
- output 6: float32 [2, 9, 64, 576], replicated
- output 7: float32 [2, 576], replicated
- output 8: float32 [2, 576, 1536], replicated
- output 9: float32 [2, 576, 1536], replicated
- output 10: float32 [2, 1536, 576], replicated
All inputs are finite; a program needn't handle non-finite values.
Results may differ from the reference program's by a relative error of at most 0.02.
Values sent between devices are 32-bit elements.
A program may use at most 1 GiB of HBM per device.

```python
import jax
import jax.numpy as jnp
from jax import lax

D_MODEL = 576
N_HEADS = 9
KV_HEADS = 3
HEAD_DIM = 64
FF_DIM = 1536
BATCH_DEV = 1
SEQ_LEN = 1024
DP_SIZE = 128
BATCH_ALL = BATCH_DEV * DP_SIZE
KV_GROUP = N_HEADS // KV_HEADS
ATT_SCALE = HEAD_DIM ** -0.5
NORM_EPS = 1e-6
ROPE_THETA = 10000.0


def setup_inputs(seed: int = 0) -> dict:
    key_list = jax.random.split(jax.random.key(seed), 15)
    act_shape = (BATCH_ALL, SEQ_LEN, D_MODEL)

    def activation(key_val, key_scale):
        seq_scale = 0.5 + jax.random.uniform(key_list[key_scale], (BATCH_ALL, 1, 1), jnp.float32)
        return (jax.random.normal(key_list[key_val], act_shape, jnp.float32) * seq_scale).astype(jnp.bfloat16)

    def matrix(key_idx, shape_w, fan_in):
        return (jax.random.normal(key_list[key_idx], shape_w, jnp.float32) * fan_in ** -0.5).astype(jnp.bfloat16)

    def gain_vec(key_idx):
        return (1.0 + 0.3 * jax.random.normal(key_list[key_idx], (2, D_MODEL), jnp.float32)).astype(jnp.bfloat16)

    return {
        "x_layer0": activation(0, 1),
        "x_layer1": activation(2, 3),
        "d_out": activation(4, 5),
        "g_attn": gain_vec(6),
        "w_q": matrix(7, (2, D_MODEL, N_HEADS, HEAD_DIM), D_MODEL),
        "w_k": matrix(8, (2, D_MODEL, KV_HEADS, HEAD_DIM), D_MODEL),
        "w_v": matrix(9, (2, D_MODEL, KV_HEADS, HEAD_DIM), D_MODEL),
        "w_o": matrix(10, (2, N_HEADS, HEAD_DIM, D_MODEL), N_HEADS * HEAD_DIM),
        "g_ffn": gain_vec(11),
        "w_gate": matrix(12, (2, D_MODEL, FF_DIM), D_MODEL),
        "w_up": matrix(13, (2, D_MODEL, FF_DIM), D_MODEL),
        "w_down": matrix(14, (2, FF_DIM, D_MODEL), FF_DIM),
    }


def rope_tables():
    positions = jnp.arange(SEQ_LEN, dtype=jnp.float32)
    inv_freq = ROPE_THETA ** (-jnp.arange(0, HEAD_DIM, 2, dtype=jnp.float32) / HEAD_DIM)
    angles = positions[:, None] * inv_freq[None, :]
    return jnp.cos(angles), jnp.sin(angles)


def rotate(values, cos_t, sin_t):
    x_pairs = values.reshape(values.shape[:-1] + (values.shape[-1] // 2, 2))
    x_even = x_pairs[..., 0]
    x_odd = x_pairs[..., 1]
    cos_b = cos_t[:, None, :]
    sin_b = sin_t[:, None, :]
    turned = jnp.stack([x_even * cos_b - x_odd * sin_b, x_even * sin_b + x_odd * cos_b], axis=-1)
    return turned.reshape(values.shape)


def as_bf16(values):
    return values.astype(jnp.bfloat16).astype(jnp.float32)


def rms_scale(x_resid, gain):
    return x_resid * lax.rsqrt(jnp.mean(x_resid * x_resid, axis=-1, keepdims=True) + NORM_EPS) * gain


def layer_forward(x_in, params):
    g_attn, w_q, w_k, w_v, w_o, g_ffn, w_gate, w_up, w_down = params
    cos_t, sin_t = rope_tables()
    x_resid = x_in.astype(jnp.float32)
    normed = as_bf16(rms_scale(x_resid, g_attn))
    q_pre = as_bf16(jnp.einsum("bsd,dnh->bsnh", normed, w_q))
    k_pre = as_bf16(jnp.einsum("bsd,dnh->bsnh", normed, w_k))
    v_act = as_bf16(jnp.einsum("bsd,dnh->bsnh", normed, w_v))
    q_rot = as_bf16(rotate(q_pre, cos_t, sin_t)).reshape(BATCH_DEV, SEQ_LEN, KV_HEADS, KV_GROUP, HEAD_DIM)
    k_rot = as_bf16(rotate(k_pre, cos_t, sin_t))
    causal = jnp.arange(SEQ_LEN)[:, None] >= jnp.arange(SEQ_LEN)[None, :]
    scores = jnp.einsum("bskgd,btkd->bkgst", q_rot, k_rot) * ATT_SCALE
    p_attn = as_bf16(jax.nn.softmax(jnp.where(causal, scores, -1e30), axis=-1))
    attn_out = as_bf16(jnp.einsum("bkgst,btkd->bskgd", p_attn, v_act)).reshape(BATCH_DEV, SEQ_LEN, N_HEADS, HEAD_DIM)
    x_mid = as_bf16(x_resid + jnp.einsum("bsnh,nhd->bsd", attn_out, w_o))
    normed_ffn = as_bf16(rms_scale(x_mid, g_ffn))
    gate_act = as_bf16(jnp.einsum("bsd,df->bsf", normed_ffn, w_gate))
    up_act = as_bf16(jnp.einsum("bsd,df->bsf", normed_ffn, w_up))
    hidden = as_bf16(jax.nn.silu(gate_act) * up_act)
    return (x_mid + jnp.einsum("bsf,fd->bsd", hidden, w_down)).astype(jnp.bfloat16)


def layer_grads(x_in, d_out, params):
    pull_back = jax.vjp(layer_forward, x_in, params)[1]
    return pull_back(d_out)


def reference(x_layer0, x_layer1, d_out, g_attn, w_q, w_k, w_v, w_o, g_ffn, w_gate, w_up, w_down):
    weights = (g_attn, w_q, w_k, w_v, w_o, g_ffn, w_gate, w_up, w_down)
    params_low = tuple(weight[0].astype(jnp.float32) for weight in weights)
    params_top = tuple(weight[1].astype(jnp.float32) for weight in weights)
    shape_dev = (DP_SIZE, BATCH_DEV, SEQ_LEN, D_MODEL)

    def one_shard(running, shard_in):
        x_zero, x_one, d_top = shard_in
        d_mid, grads_top = layer_grads(x_one, d_top, params_top)
        d_first, grads_low = layer_grads(x_zero, d_mid, params_low)
        running = tuple(run_sum + jnp.stack([low_grad, top_grad]) for run_sum, low_grad, top_grad in zip(running, grads_low, grads_top))
        return running, d_first

    zero_grads = tuple(jnp.zeros(weight.shape, jnp.float32) for weight in weights)
    grad_sums, dx_shards = lax.scan(one_shard, zero_grads, (x_layer0.reshape(shape_dev), x_layer1.reshape(shape_dev), d_out.reshape(shape_dev)))
    dx_layer0 = dx_shards.reshape(BATCH_ALL, SEQ_LEN, D_MODEL)
    return (dx_layer0, grad_sums[0] / DP_SIZE, grad_sums[1] / DP_SIZE, grad_sums[2] / DP_SIZE, grad_sums[3] / DP_SIZE, grad_sums[4] / DP_SIZE, grad_sums[5] / DP_SIZE, grad_sums[6] / DP_SIZE, grad_sums[7] / DP_SIZE, grad_sums[8] / DP_SIZE)
```

```python
import functools

import jax
import jax.numpy as jnp
import numpy as np
from jax import lax
from jax.experimental import pallas as pl
from jax.experimental.pallas import tpu as pltpu
from jax.sharding import PartitionSpec as P

NORM_EPS = 1e-6
ROPE_THETA = 10000.0
BLK = 256
LOG2E = 1.4426950408889634
F32 = jnp.float32
BF16 = jnp.bfloat16


def rope_tables_np(seq_len, head_dim):
    positions = np.arange(seq_len, dtype=np.float32)
    inv_freq = np.float32(ROPE_THETA) ** (-np.arange(0, head_dim, 2, dtype=np.float32) / np.float32(head_dim))
    angles = (positions[None, :] * inv_freq.astype(np.float32)[:, None]).astype(np.float32)
    cos_t = np.repeat(np.cos(angles), 2, axis=0).astype(np.float32)
    sin_t = np.repeat(np.sin(angles), 2, axis=0).astype(np.float32)
    sin_t[0::2] *= -1.0
    return cos_t, sin_t


def pair_swap(values):
    rows = values.shape[0]
    even = lax.broadcasted_iota(jnp.int32, values.shape, 0) % 2 == 0
    return jnp.where(even, pltpu.roll(values, rows - 1, 0), pltpu.roll(values, 1, 0))


def dot_nn(lhs, rhs):
    return lax.dot_general(lhs, rhs, (((1,), (0,)), ((), ())), preferred_element_type=F32)


def dot_nt(lhs, rhs):
    return lax.dot_general(lhs, rhs, (((1,), (1,)), ((), ())), preferred_element_type=F32)


def diag_mask():
    keys = lax.broadcasted_iota(jnp.int32, (BLK, BLK), 0)
    queries = lax.broadcasted_iota(jnp.int32, (BLK, BLK), 1)
    return queries >= keys


def attn_fwd_kernel(n_group, head_dim, att_scale, q_ref, k_ref, v_ref, cos_ref, sin_ref, a_ref, qr_ref, kr_ref, st_ref, k_scr):
    seq_len = k_ref.shape[1]
    n_blk = seq_len // BLK
    cos_t = cos_ref[...]
    sin_t = sin_ref[...]
    k_f = k_ref[...].astype(F32)
    k_rot = (k_f * cos_t + pair_swap(k_f) * sin_t).astype(BF16)
    kr_ref[...] = k_rot
    k_scr[...] = k_rot.astype(F32).T.astype(BF16)
    coef = att_scale * LOG2E
    mask = diag_mask()
    st_ref[...] = jnp.zeros_like(st_ref)
    for head in range(n_group):
        rows = slice(head * head_dim, (head + 1) * head_dim)
        q_f = q_ref[rows, :].astype(F32)
        qr_ref[rows, :] = (q_f * cos_t + pair_swap(q_f) * sin_t).astype(BF16)
        for j in range(n_blk):
            cols = slice(j * BLK, (j + 1) * BLK)
            q_j = qr_ref[rows, cols]
            s_blocks = []
            for i in range(j + 1):
                s_i = dot_nn(k_scr[i * BLK:(i + 1) * BLK, :], q_j)
                if i == j:
                    s_i = jnp.where(mask, s_i, -1e30)
                s_blocks.append(s_i)
            top = functools.reduce(jnp.maximum, [jnp.max(s_i, axis=0, keepdims=True) for s_i in s_blocks])
            e_blocks = [jnp.exp2((s_i - top) * coef) for s_i in s_blocks]
            total = functools.reduce(jnp.add, [jnp.sum(e_i, axis=0, keepdims=True) for e_i in e_blocks])
            inv = 1.0 / total
            acc = None
            for i in range(j + 1):
                p_i = (e_blocks[i] * inv).astype(BF16)
                part = dot_nn(v_ref[:, i * BLK:(i + 1) * BLK], p_i)
                acc = part if acc is None else acc + part
            a_ref[rows, cols] = acc.astype(BF16)
            st_ref[0, head:head + 1, cols] = top
            st_ref[0, n_group + head:n_group + head + 1, cols] = inv


def attn_bwd_kernel(n_group, head_dim, att_scale, qr_ref, kr_ref, v_ref, do_ref, st_ref, cos_ref, sin_ref, dq_ref, dk_ref, dv_ref, k_scr, v_scr, dk_acc, dv_acc):
    seq_len = kr_ref.shape[1]
    n_blk = seq_len // BLK
    k_scr[...] = kr_ref[...].astype(F32).T.astype(BF16)
    v_scr[...] = v_ref[...].astype(F32).T.astype(BF16)
    dk_acc[...] = jnp.zeros_like(dk_acc)
    dv_acc[...] = jnp.zeros_like(dv_acc)
    coef = att_scale * LOG2E
    mask = diag_mask()
    for head in range(n_group):
        rows = slice(head * head_dim, (head + 1) * head_dim)
        for j in range(n_blk):
            cols = slice(j * BLK, (j + 1) * BLK)
            q_j = qr_ref[rows, cols]
            do_j = do_ref[rows, cols]
            top = st_ref[0, head:head + 1, cols]
            inv = st_ref[0, n_group + head:n_group + head + 1, cols]
            p_blocks = []
            dp_blocks = []
            row_dot = None
            for i in range(j + 1):
                keys = slice(i * BLK, (i + 1) * BLK)
                s_i = dot_nn(k_scr[keys, :], q_j)
                if i == j:
                    s_i = jnp.where(mask, s_i, -1e30)
                p_i = jnp.exp2((s_i - top) * coef) * inv
                dp_i = dot_nn(v_scr[keys, :], do_j).astype(BF16).astype(F32)
                part = jnp.sum(p_i * dp_i, axis=0, keepdims=True)
                row_dot = part if row_dot is None else row_dot + part
                dv_acc[:, keys] += dot_nt(do_j, p_i.astype(BF16))
                p_blocks.append(p_i)
                dp_blocks.append(dp_i)
            dq_j = None
            for i in range(j + 1):
                keys = slice(i * BLK, (i + 1) * BLK)
                ds_i = (p_blocks[i] * (dp_blocks[i] - row_dot) * att_scale).astype(BF16)
                part = dot_nn(kr_ref[:, keys], ds_i)
                dq_j = part if dq_j is None else dq_j + part
                dk_acc[:, keys] += dot_nt(q_j, ds_i)
            dq_j = dq_j.astype(BF16).astype(F32)
            dq_ref[rows, cols] = (dq_j * cos_ref[:, cols] - pair_swap(dq_j) * sin_ref[:, cols]).astype(BF16)
    d_k = dk_acc[...].astype(BF16).astype(F32)
    dk_ref[...] = (d_k * cos_ref[...] - pair_swap(d_k) * sin_ref[...]).astype(BF16)
    dv_ref[...] = dv_acc[...].astype(BF16)


def attn_specs(kv_heads, n_group, head_dim, seq_len):
    q_spec = pl.BlockSpec((n_group * head_dim, seq_len), lambda g: (g, 0))
    kv_spec = pl.BlockSpec((head_dim, seq_len), lambda g: (g, 0))
    tab_spec = pl.BlockSpec((head_dim, seq_len), lambda g: (0, 0))
    st_spec = pl.BlockSpec((1, 8, seq_len), lambda g: (g, 0, 0))
    return q_spec, kv_spec, tab_spec, st_spec


def attn_forward(q_t, k_t, v_t, cos_t, sin_t, kv_heads, head_dim):
    seq_len = q_t.shape[1]
    n_group = q_t.shape[0] // k_t.shape[0]
    q_spec, kv_spec, tab_spec, st_spec = attn_specs(kv_heads, n_group, head_dim, seq_len)
    flops = 2 * 2 * q_t.shape[0] * seq_len * seq_len
    return pl.pallas_call(
        functools.partial(attn_fwd_kernel, n_group, head_dim, head_dim ** -0.5),
        grid=(kv_heads,),
        in_specs=[q_spec, kv_spec, kv_spec, tab_spec, tab_spec],
        out_specs=[q_spec, q_spec, kv_spec, st_spec],
        out_shape=[jax.ShapeDtypeStruct(q_t.shape, BF16), jax.ShapeDtypeStruct(q_t.shape, BF16), jax.ShapeDtypeStruct(k_t.shape, BF16), jax.ShapeDtypeStruct((kv_heads, 8, seq_len), F32)],
        scratch_shapes=[pltpu.VMEM((seq_len, head_dim), BF16)],
        compiler_params=pltpu.CompilerParams(vmem_limit_bytes=40 * 1024 * 1024),
        cost_estimate=pl.CostEstimate(flops=8 * flops, bytes_accessed=8 * q_t.size, transcendentals=0),
        name="attn_fwd",
    )(q_t, k_t, v_t, cos_t, sin_t)


def attn_backward(qr_t, kr_t, v_t, do_t, stats, cos_t, sin_t, kv_heads, head_dim):
    seq_len = qr_t.shape[1]
    n_group = qr_t.shape[0] // kr_t.shape[0]
    q_spec, kv_spec, tab_spec, st_spec = attn_specs(kv_heads, n_group, head_dim, seq_len)
    flops = 5 * 2 * qr_t.shape[0] * seq_len * seq_len
    return pl.pallas_call(
        functools.partial(attn_bwd_kernel, n_group, head_dim, head_dim ** -0.5),
        grid=(kv_heads,),
        in_specs=[q_spec, kv_spec, kv_spec, q_spec, st_spec, tab_spec, tab_spec],
        out_specs=[q_spec, kv_spec, kv_spec],
        out_shape=[jax.ShapeDtypeStruct(qr_t.shape, BF16), jax.ShapeDtypeStruct(kr_t.shape, BF16), jax.ShapeDtypeStruct(kr_t.shape, BF16)],
        scratch_shapes=[pltpu.VMEM((seq_len, head_dim), BF16), pltpu.VMEM((seq_len, head_dim), BF16), pltpu.VMEM((head_dim, seq_len), F32), pltpu.VMEM((head_dim, seq_len), F32)],
        compiler_params=pltpu.CompilerParams(vmem_limit_bytes=48 * 1024 * 1024),
        cost_estimate=pl.CostEstimate(flops=8 * flops, bytes_accessed=8 * qr_t.size, transcendentals=0),
        name="attn_bwd",
    )(qr_t, kr_t, v_t, do_t, stats, cos_t, sin_t)


def dot_c(lhs, rhs, c_l, c_r):
    return lax.dot_general(lhs, rhs, (((c_l,), (c_r,)), ((), ())), preferred_element_type=F32)


def norm_back_t(x_f, inv_rms, gain, d_normed):
    scaled = d_normed * gain
    d_resid = inv_rms * scaled - x_f * (inv_rms ** 3) * jnp.mean(scaled * x_f, axis=0, keepdims=True)
    d_gain = jnp.sum(d_normed * x_f * inv_rms, axis=1)
    return d_resid, d_gain


def layer_forward_t(x_t, weights, cos_t, sin_t, kv_heads, head_dim):
    g_attn, wq_t, wk_t, wv_t, w_o, g_ffn, w_gate, w_up, wd_t = weights
    x_f = x_t.astype(F32)
    inv_attn = lax.rsqrt(jnp.mean(x_f * x_f, axis=0, keepdims=True) + NORM_EPS)
    normed = (x_f * inv_attn * g_attn.astype(F32)[:, None]).astype(BF16)
    q_t = dot_c(wq_t, normed, 1, 0).astype(BF16)
    k_t = dot_c(wk_t, normed, 1, 0).astype(BF16)
    v_t = dot_c(wv_t, normed, 1, 0).astype(BF16)
    a_t, qr_t, kr_t, stats = attn_forward(q_t, k_t, v_t, cos_t, sin_t, kv_heads, head_dim)
    m_t = (x_f + dot_c(w_o, a_t, 0, 0)).astype(BF16)
    m_f = m_t.astype(F32)
    inv_ffn = lax.rsqrt(jnp.mean(m_f * m_f, axis=0, keepdims=True) + NORM_EPS)
    normed_ffn = (m_f * inv_ffn * g_ffn.astype(F32)[:, None]).astype(BF16)
    gate_t = dot_c(w_gate, normed_ffn, 0, 0).astype(BF16)
    up_t = dot_c(w_up, normed_ffn, 0, 0).astype(BF16)
    return x_f, inv_attn, normed, v_t, a_t, qr_t, kr_t, stats, m_f, inv_ffn, normed_ffn, gate_t, up_t


def layer_backward_t(saved, d_out_t, weights, cos_t, sin_t, kv_heads, head_dim, scale):
    g_attn, wq_t, wk_t, wv_t, w_o, g_ffn, w_gate, w_up, wd_t = weights
    x_f, inv_attn, normed, v_t, a_t, qr_t, kr_t, stats, m_f, inv_ffn, normed_ffn, gate_t, up_t = saved
    gate_f = gate_t.astype(F32)
    gate_sig = jax.nn.sigmoid(gate_f)
    silu_act = gate_f * gate_sig
    up_f = up_t.astype(F32)
    hidden = (silu_act * up_f).astype(BF16)
    grad_wd_t = dot_c(d_out_t, hidden, 1, 1) * scale
    d_hidden = dot_c(wd_t, d_out_t, 0, 0).astype(BF16).astype(F32)
    d_gate = (d_hidden * up_f * gate_sig * (1.0 + gate_f * (1.0 - gate_sig))).astype(BF16)
    d_up = (d_hidden * silu_act).astype(BF16)
    grad_w_gate = dot_c(normed_ffn, d_gate, 1, 1) * scale
    grad_w_up = dot_c(normed_ffn, d_up, 1, 1) * scale
    d_normed_ffn = (dot_c(w_gate, d_gate, 1, 0) + dot_c(w_up, d_up, 1, 0)).astype(BF16).astype(F32)
    d_mid_norm, grad_g_ffn = norm_back_t(m_f, inv_ffn, g_ffn.astype(F32)[:, None], d_normed_ffn)
    d_mid = (d_out_t.astype(F32) + d_mid_norm).astype(BF16)
    grad_w_o = dot_c(a_t, d_mid, 1, 1) * scale
    d_attn = dot_c(w_o, d_mid, 1, 0).astype(BF16)
    dq_t, dk_t, dv_t = attn_backward(qr_t, kr_t, v_t, d_attn, stats, cos_t, sin_t, kv_heads, head_dim)
    grad_wq_t = dot_c(dq_t, normed, 1, 1) * scale
    grad_wk_t = dot_c(dk_t, normed, 1, 1) * scale
    grad_wv_t = dot_c(dv_t, normed, 1, 1) * scale
    d_normed = (dot_c(wq_t, dq_t, 0, 0) + dot_c(wk_t, dk_t, 0, 0) + dot_c(wv_t, dv_t, 0, 0)).astype(BF16).astype(F32)
    d_x_norm, grad_g_attn = norm_back_t(x_f, inv_attn, g_attn.astype(F32)[:, None], d_normed)
    d_x = (d_mid.astype(F32) + d_x_norm).astype(BF16)
    return d_x, (grad_wd_t, grad_w_gate, grad_w_up, grad_w_o, grad_wq_t, grad_wk_t, grad_wv_t, grad_g_attn * scale, grad_g_ffn * scale)


def solution(mesh):
    num_devices = mesh.shape["dp"]
    act_spec = P("dp", None, None)
    rep_spec = P()

    def local_step(x_layer0, x_layer1, d_out, g_attn, w_q, w_k, w_v, w_o, g_ffn, w_gate, w_up, w_down):
        _, seq_len, model_dim = x_layer0.shape
        n_heads, head_dim = w_q.shape[2], w_q.shape[3]
        kv_heads = w_k.shape[2]
        cos_np, sin_np = rope_tables_np(seq_len, head_dim)
        cos_t, sin_t = jnp.asarray(cos_np), jnp.asarray(sin_np)
        scale = 1.0 / num_devices

        def layer_weights(layer):
            def heads_out(w):
                return jnp.transpose(w[layer], (1, 2, 0)).reshape(-1, model_dim)
            return (g_attn[layer], heads_out(w_q), heads_out(w_k), heads_out(w_v), w_o[layer].reshape(-1, model_dim), g_ffn[layer], w_gate[layer], w_up[layer], jnp.transpose(w_down[layer], (1, 0)))

        x0_t = jnp.transpose(x_layer0[0], (1, 0))
        x1_t = jnp.transpose(x_layer1[0], (1, 0))
        d_top = jnp.transpose(d_out[0], (1, 0))
        w_low, w_top = layer_weights(0), layer_weights(1)
        saved_top = layer_forward_t(x1_t, w_top, cos_t, sin_t, kv_heads, head_dim)
        d_mid, grads_top = layer_backward_t(saved_top, d_top, w_top, cos_t, sin_t, kv_heads, head_dim, scale)
        saved_low = layer_forward_t(x0_t, w_low, cos_t, sin_t, kv_heads, head_dim)
        d_x0, grads_low = layer_backward_t(saved_low, d_mid, w_low, cos_t, sin_t, kv_heads, head_dim, scale)
        stacked = [jnp.stack([low, top]) for low, top in zip(grads_low, grads_top)]
        gd, gg, gu, go, gq, gk, gv, g1, g2 = stacked
        big_o = jnp.concatenate([go, jnp.zeros((2, 8, model_dim), F32).at[:, 0].set(g1).at[:, 1].set(g2)], axis=1)
        gd, gg, gu, big_o, gq, gk, gv = lax.psum((gd, gg, gu, big_o, gq, gk, gv), "dp")
        go = big_o[:, :n_heads * head_dim]
        g1 = big_o[:, n_heads * head_dim]
        g2 = big_o[:, n_heads * head_dim + 1]

        def heads_in(g):
            return jnp.transpose(g.reshape(2, -1, head_dim, model_dim), (0, 3, 1, 2))

        d_x = jnp.transpose(d_x0, (1, 0))[None]
        return (d_x, g1, heads_in(gq), heads_in(gk), heads_in(gv), go.reshape(2, n_heads, head_dim, model_dim), g2, gg, gu, jnp.transpose(gd, (0, 2, 1)))

    return jax.shard_map(local_step, mesh=mesh, in_specs=(act_spec, act_spec, act_spec) + (rep_spec,) * 9, out_specs=(act_spec,) + (rep_spec,) * 9, check_vma=False)
```

```python
import functools

import jax
import jax.numpy as jnp
import numpy as np
from jax import lax
from jax.experimental import pallas as pl
from jax.experimental.pallas import tpu as pltpu
from jax.sharding import PartitionSpec as P

NORM_EPS = 1e-6
ROPE_THETA = 10000.0
BLK = 256
LOG2E = 1.4426950408889634
F32 = jnp.float32
BF16 = jnp.bfloat16


def rope_tables_np(seq_len, head_dim):
    positions = np.arange(seq_len, dtype=np.float32)
    inv_freq = np.float32(ROPE_THETA) ** (-np.arange(0, head_dim, 2, dtype=np.float32) / np.float32(head_dim))
    angles = (positions[None, :] * inv_freq.astype(np.float32)[:, None]).astype(np.float32)
    cos_t = np.repeat(np.cos(angles), 2, axis=0).astype(np.float32)
    sin_t = np.repeat(np.sin(angles), 2, axis=0).astype(np.float32)
    sin_t[0::2] *= -1.0
    return cos_t, sin_t


def pair_swap(values):
    rows = values.shape[0]
    even = lax.broadcasted_iota(jnp.int32, values.shape, 0) % 2 == 0
    return jnp.where(even, pltpu.roll(values, rows - 1, 0), pltpu.roll(values, 1, 0))


def dot_nn(lhs, rhs):
    return lax.dot_general(lhs, rhs, (((1,), (0,)), ((), ())), preferred_element_type=F32)


def dot_nt(lhs, rhs):
    return lax.dot_general(lhs, rhs, (((1,), (1,)), ((), ())), preferred_element_type=F32)


def diag_mask():
    keys = lax.broadcasted_iota(jnp.int32, (BLK, BLK), 0)
    queries = lax.broadcasted_iota(jnp.int32, (BLK, BLK), 1)
    return queries >= keys


def attn_fwd_kernel(n_group, head_dim, att_scale, qkv_ref, cos_ref, sin_ref, a_ref, rot_ref, st_ref, k_scr):
    seq_len = qkv_ref.shape[1]
    n_blk = seq_len // BLK
    q_rows = n_group * head_dim
    cos_t = cos_ref[...]
    sin_t = sin_ref[...]
    k_f = qkv_ref[q_rows:q_rows + head_dim, :].astype(F32)
    k_rot = (k_f * cos_t + pair_swap(k_f) * sin_t).astype(BF16)
    rot_ref[q_rows:q_rows + head_dim, :] = k_rot
    k_scr[...] = k_rot.astype(F32).T.astype(BF16)
    coef = att_scale * LOG2E
    mask = diag_mask()
    st_ref[...] = jnp.zeros_like(st_ref)
    for head in range(n_group):
        rows = slice(head * head_dim, (head + 1) * head_dim)
        q_f = qkv_ref[rows, :].astype(F32)
        rot_ref[rows, :] = (q_f * cos_t + pair_swap(q_f) * sin_t).astype(BF16)
        for j in range(n_blk):
            cols = slice(j * BLK, (j + 1) * BLK)
            q_j = rot_ref[rows, cols]
            s_blocks = []
            for i in range(j + 1):
                s_i = dot_nn(k_scr[i * BLK:(i + 1) * BLK, :], q_j)
                if i == j:
                    s_i = jnp.where(mask, s_i, -1e30)
                s_blocks.append(s_i)
            top = functools.reduce(jnp.maximum, [jnp.max(s_i, axis=0, keepdims=True) for s_i in s_blocks])
            e_blocks = [jnp.exp2((s_i - top) * coef) for s_i in s_blocks]
            total = functools.reduce(jnp.add, [jnp.sum(e_i, axis=0, keepdims=True) for e_i in e_blocks])
            inv = 1.0 / total
            acc = None
            for i in range(j + 1):
                p_i = (e_blocks[i] * inv).astype(BF16)
                part = dot_nn(qkv_ref[q_rows + head_dim:q_rows + 2 * head_dim, i * BLK:(i + 1) * BLK], p_i)
                acc = part if acc is None else acc + part
            a_ref[rows, cols] = acc.astype(BF16)
            st_ref[0, head:head + 1, cols] = top
            st_ref[0, n_group + head:n_group + head + 1, cols] = inv


def attn_bwd_kernel(n_group, head_dim, att_scale, rot_ref, v_ref, do_ref, st_ref, cos_ref, sin_ref, dqkv_ref, k_scr, v_scr, dk_acc, dv_acc):
    seq_len = rot_ref.shape[1]
    n_blk = seq_len // BLK
    q_rows = n_group * head_dim
    k_rows = slice(q_rows, q_rows + head_dim)
    k_scr[...] = rot_ref[k_rows, :].astype(F32).T.astype(BF16)
    v_scr[...] = v_ref[...].astype(F32).T.astype(BF16)
    dk_acc[...] = jnp.zeros_like(dk_acc)
    dv_acc[...] = jnp.zeros_like(dv_acc)
    coef = att_scale * LOG2E
    mask = diag_mask()
    for head in range(n_group):
        rows = slice(head * head_dim, (head + 1) * head_dim)
        for j in range(n_blk):
            cols = slice(j * BLK, (j + 1) * BLK)
            q_j = rot_ref[rows, cols]
            do_j = do_ref[rows, cols]
            top = st_ref[0, head:head + 1, cols]
            inv = st_ref[0, n_group + head:n_group + head + 1, cols]
            p_blocks = []
            dp_blocks = []
            row_dot = None
            for i in range(j + 1):
                keys = slice(i * BLK, (i + 1) * BLK)
                s_i = dot_nn(k_scr[keys, :], q_j)
                if i == j:
                    s_i = jnp.where(mask, s_i, -1e30)
                p_i = jnp.exp2((s_i - top) * coef) * inv
                dp_i = dot_nn(v_scr[keys, :], do_j).astype(BF16).astype(F32)
                part = jnp.sum(p_i * dp_i, axis=0, keepdims=True)
                row_dot = part if row_dot is None else row_dot + part
                dv_acc[:, keys] += dot_nt(do_j, p_i.astype(BF16))
                p_blocks.append(p_i)
                dp_blocks.append(dp_i)
            dq_j = None
            for i in range(j + 1):
                keys = slice(i * BLK, (i + 1) * BLK)
                ds_i = (p_blocks[i] * (dp_blocks[i] - row_dot) * att_scale).astype(BF16)
                part = dot_nn(rot_ref[k_rows, keys], ds_i)
                dq_j = part if dq_j is None else dq_j + part
                dk_acc[:, keys] += dot_nt(q_j, ds_i)
            dq_j = dq_j.astype(BF16).astype(F32)
            dqkv_ref[rows, cols] = (dq_j * cos_ref[:, cols] - pair_swap(dq_j) * sin_ref[:, cols]).astype(BF16)
    d_k = dk_acc[...].astype(BF16).astype(F32)
    dqkv_ref[k_rows, :] = (d_k * cos_ref[...] - pair_swap(d_k) * sin_ref[...]).astype(BF16)
    dqkv_ref[q_rows + head_dim:q_rows + 2 * head_dim, :] = dv_acc[...].astype(BF16)


def attn_forward(qkv_t, cos_t, sin_t, kv_heads, n_group, head_dim):
    seq_len = qkv_t.shape[1]
    per = (n_group + 2) * head_dim
    tab_spec = pl.BlockSpec((head_dim, seq_len), lambda g: (0, 0))
    flops = 2 * 2 * kv_heads * n_group * head_dim * seq_len * seq_len
    return pl.pallas_call(
        functools.partial(attn_fwd_kernel, n_group, head_dim, head_dim ** -0.5),
        grid=(kv_heads,),
        in_specs=[pl.BlockSpec((per, seq_len), lambda g: (g, 0)), tab_spec, tab_spec],
        out_specs=[pl.BlockSpec((n_group * head_dim, seq_len), lambda g: (g, 0)), pl.BlockSpec(((n_group + 1) * head_dim, seq_len), lambda g: (g, 0)), pl.BlockSpec((1, 8, seq_len), lambda g: (g, 0, 0))],
        out_shape=[jax.ShapeDtypeStruct((kv_heads * n_group * head_dim, seq_len), BF16), jax.ShapeDtypeStruct((kv_heads * (n_group + 1) * head_dim, seq_len), BF16), jax.ShapeDtypeStruct((kv_heads, 8, seq_len), F32)],
        scratch_shapes=[pltpu.VMEM((seq_len, head_dim), BF16)],
        compiler_params=pltpu.CompilerParams(vmem_limit_bytes=40 * 1024 * 1024),
        cost_estimate=pl.CostEstimate(flops=8 * flops, bytes_accessed=8 * qkv_t.size, transcendentals=0),
        name="attn_fwd",
    )(qkv_t, cos_t, sin_t)


def attn_backward(rot_t, qkv_t, do_t, stats, cos_t, sin_t, kv_heads, n_group, head_dim):
    seq_len = qkv_t.shape[1]
    per = (n_group + 2) * head_dim
    tab_spec = pl.BlockSpec((head_dim, seq_len), lambda g: (0, 0))
    flops = 5 * 2 * kv_heads * n_group * head_dim * seq_len * seq_len
    return pl.pallas_call(
        functools.partial(attn_bwd_kernel, n_group, head_dim, head_dim ** -0.5),
        grid=(kv_heads,),
        in_specs=[
            pl.BlockSpec(((n_group + 1) * head_dim, seq_len), lambda g: (g, 0)),
            pl.BlockSpec((head_dim, seq_len), lambda g: (g * (n_group + 2) + n_group + 1, 0)),
            pl.BlockSpec((n_group * head_dim, seq_len), lambda g: (g, 0)),
            pl.BlockSpec((1, 8, seq_len), lambda g: (g, 0, 0)),
            tab_spec,
            tab_spec,
        ],
        out_specs=pl.BlockSpec((per, seq_len), lambda g: (g, 0)),
        out_shape=jax.ShapeDtypeStruct(qkv_t.shape, BF16),
        scratch_shapes=[pltpu.VMEM((seq_len, head_dim), BF16), pltpu.VMEM((seq_len, head_dim), BF16), pltpu.VMEM((head_dim, seq_len), F32), pltpu.VMEM((head_dim, seq_len), F32)],
        compiler_params=pltpu.CompilerParams(vmem_limit_bytes=48 * 1024 * 1024),
        cost_estimate=pl.CostEstimate(flops=8 * flops, bytes_accessed=8 * qkv_t.size, transcendentals=0),
        name="attn_bwd",
    )(rot_t, qkv_t, do_t, stats, cos_t, sin_t)


MESH = pl.DeviceIdType.MESH
N_RED = 3
N_ICI = 6


def add_rows(dst, src, rows, step):
    @pl.loop(0, rows // step)
    def _(i):
        part = pl.ds(pl.multiple_of(i * step, 8), step)
        dst[part, :] = dst[part, :] + src[part, :]


def all_reduce_kernel(a_rows, a_lanes, q_rows, o_rows, *refs):
    srcs = [refs[5 * layer:5 * layer + 5] for layer in range(2)]
    gain_ref = refs[10]
    out_a, out_q, out_o, out_g = refs[11:15]
    acc_a, acc_b = refs[15:17]
    bufs_a = refs[17:24]
    bufs_b = refs[24:31]
    gain_bufs = refs[31]
    (core_send, core_recv, load_sem, ici_send, ici_recv, ag_send, ag_recv, fin_send, fin_recv, fin_loc, g_send, g_recv, g_loc) = refs[32:45]

    me = lax.axis_index("dp")
    core = lax.rem(me, 2)
    coords = (lax.rem(me // 2, 4), lax.rem(me // 8, 4), me // 32)
    strides = (2, 8, 32)
    peer = me + 1 - 2 * core
    gens = []
    for kind in range(2):
        for axis in range(3):
            v = coords[axis]
            if kind == 0:
                partner, bit = v + 1 - 2 * lax.rem(v, 2), lax.rem(v + v // 2, 2)
            else:
                partner, bit = 3 - v, v // 2
            gens.append((me + (partner - v) * strides[axis], bit))

    barrier = pltpu.get_barrier_semaphore()
    for dev in [peer] + [g[0] for g in gens]:
        pl.semaphore_signal(barrier, inc=1, device_id=(dev,), device_id_type=MESH)
    pl.semaphore_wait(barrier, 1 + N_ICI)

    half = a_rows // 2
    lanes = a_lanes // 2
    o_half = o_rows // 12
    q_half = q_rows // 12
    b_rows = o_half + q_half

    def ds8(start, size):
        return pl.ds(pl.multiple_of(start, 8), size)

    def remote(src, dst, send, recv, dev):
        return pltpu.make_async_remote_copy(src_ref=src, dst_ref=dst, send_sem=send, recv_sem=recv, device_id=(dev,), device_id_type=MESH)

    flows = [(layer, k) for layer in (1, 0) for k in range(6)]
    core_copies = {}
    load_copies = {}
    for layer, k in flows:
        mat = srcs[layer][k // 2]
        q_src, o_src = srcs[layer][3:]
        lane = slice((k % 2) * lanes, (k % 2 + 1) * lanes)

        def parts(which):
            return (
                (mat.at[ds8(which * half, half), lane], lambda buf_a, buf_b: buf_a.at[layer, k]),
                (o_src.at[ds8(k * 2 * o_half + which * o_half, o_half), :], lambda buf_a, buf_b: buf_b.at[layer, k, 0:o_half, :]),
                (q_src.at[ds8(k * 2 * q_half + which * q_half, q_half), :], lambda buf_a, buf_b: buf_b.at[layer, k, o_half:b_rows, :]),
            )

        sends = [remote(src, dst(bufs_a[0], bufs_b[0]), core_send.at[layer, k, p], core_recv.at[layer, k, p], peer) for p, (src, dst) in enumerate(parts(1 - core))]
        loads = [pltpu.make_async_copy(src, dst(acc_a, acc_b), load_sem.at[layer, k, p]) for p, (src, dst) in enumerate(parts(core))]
        for copy in sends + loads:
            copy.start()
        core_copies[layer, k] = sends
        load_copies[layer, k] = loads
    gain_copy = remote(gain_ref, gain_bufs.at[0], g_send.at[0], g_recv.at[0], peer)
    gain_copy.start()

    def part_a(step, buf, bit_keep):
        if step == 0:
            return buf.at[ds8(bit_keep * (half // 2), half // 2), :]
        if step == 1:
            return buf.at[ds8(bit_keep * (half // 4), half // 4), :]
        return buf.at[:, pl.ds(pl.multiple_of(bit_keep * (lanes // 2), 128), lanes // 2)]

    def part_b(step, buf, bit_keep):
        size = b_rows >> (step + 1)
        return buf.at[ds8(bit_keep * size, size), :]

    a_size = [half, half // 2, half // 4] + [half // 4] * 4
    b_size = [b_rows >> min(step, N_RED) for step in range(N_ICI + 1)]
    a_step = 24
    ici_copies = {}
    pending = []

    def flush():
        while pending:
            for copy in pending.pop(0):
                copy.start()

    for step in range(N_ICI + 1):
        for layer, k in flows:
            cur_a, cur_b = bufs_a[step].at[layer, k], bufs_b[step].at[layer, k]
            if step == 0:
                for copy in load_copies[layer, k]:
                    copy.wait()
                for copy in core_copies[layer, k]:
                    copy.wait_recv()
                old_a, old_b = acc_a.at[layer, k], acc_b.at[layer, k]
            else:
                for copy in ici_copies[layer, k, step - 1]:
                    copy.wait_recv()
                old_a, old_b = bufs_a[step - 1].at[layer, k], bufs_b[step - 1].at[layer, k]
                if step <= N_RED:
                    bit = gens[(k + step - 1) % N_ICI][1]
                    old_a, old_b = part_a(step - 1, old_a, bit), part_b(step - 1, old_b, bit)
            add_rows(cur_a, old_a, a_size[step], a_step)
            add_rows(cur_b, old_b, b_size[step], 16)
            if step < N_ICI:
                dev, bit = gens[(k + step) % N_ICI]
                src_a, src_b = cur_a, cur_b
                if step < N_RED:
                    src_a, src_b = part_a(step, cur_a, 1 - bit), part_b(step, cur_b, 1 - bit)
                copies = [
                    remote(src_a, bufs_a[step + 1].at[layer, k], ici_send.at[layer, k, step, 0], ici_recv.at[layer, k, step, 0], dev),
                    remote(src_b, bufs_b[step + 1].at[layer, k], ici_send.at[layer, k, step, 1], ici_recv.at[layer, k, step, 1], dev),
                ]
                ici_copies[layer, k, step] = copies
                flush()
                pending.append(copies)
        flush()
        gain_copy.wait()
        gain_old = gain_ref if step == 0 else gain_bufs.at[step - 1]
        gain_bufs[step, :, :] = gain_bufs[step, :, :] + gain_old[...]
        if step < N_ICI:
            gain_copy = remote(gain_bufs.at[step], gain_bufs.at[step + 1], g_send.at[step + 1], g_recv.at[step + 1], gens[step][0])
            gain_copy.start()
    gain_out = pltpu.make_async_copy(gain_bufs.at[N_ICI], out_g, g_loc)
    gain_out.start()

    def ag_region(layer, k, step):
        bits = [gens[(k + s) % N_ICI][1] for s in range(N_RED)]
        a_off = sum([bits[s] * (half >> (s + 1)) for s in range(min(step, 1) + 1)])
        b_off = sum([bits[s] * (b_rows >> (s + 1)) for s in range(step + 1)])
        a_cnt = half >> (min(step, 1) + 1)
        view_a = acc_a.at[layer, k, ds8(a_off, a_cnt), :]
        if step == 2:
            view_a = acc_a.at[layer, k, ds8(a_off, a_cnt), pl.ds(pl.multiple_of(bits[2] * (lanes // 2), 128), lanes // 2)]
        return view_a, acc_b.at[layer, k, ds8(b_off, b_rows >> (step + 1)), :]

    ag_copies = {}
    for step in reversed(range(N_RED)):
        for layer, k in flows:
            view_a, view_b = ag_region(layer, k, step)
            if step == N_RED - 1:
                last_a, last_b = bufs_a[N_ICI], bufs_b[N_ICI]
                view_a[...] = last_a[layer, k, :, :]
                view_b[...] = last_b[layer, k, :, :]
            else:
                for copy in ag_copies[layer, k, step + 1]:
                    copy.wait_recv()
            dev = gens[(k + step) % N_ICI][0]
            copies = [
                remote(view_a, view_a, ag_send.at[layer, k, step, 0], ag_recv.at[layer, k, step, 0], dev),
                remote(view_b, view_b, ag_send.at[layer, k, step, 1], ag_recv.at[layer, k, step, 1], dev),
            ]
            ag_copies[layer, k, step] = copies
            flush()
            pending.append(copies)
        flush()

    finals = []
    for layer, k in flows:
        for copy in ag_copies[layer, k, 0]:
            copy.wait_recv()
        lane = slice((k % 2) * lanes, (k % 2 + 1) * lanes)
        moves = [
            (acc_a.at[layer, k], out_a.at[layer, k // 2, ds8(core * half, half), lane]),
            (acc_b.at[layer, k, 0:o_half, :], out_o.at[layer, ds8(k * 2 * o_half + core * o_half, o_half), :]),
            (acc_b.at[layer, k, o_half:b_rows, :], out_q.at[layer, ds8(k * 2 * q_half + core * q_half, q_half), :]),
        ]
        for p, (src, dst) in enumerate(moves):
            far = remote(src, dst, fin_send.at[layer, k, p], fin_recv.at[layer, k, p], peer)
            near = pltpu.make_async_copy(src, dst, fin_loc.at[layer, k, p])
            far.start()
            near.start()
            finals.append((far, near))
    gain_out.wait()
    for copies in core_copies.values():
        for copy in copies:
            copy.wait_send()
    for copies in list(ici_copies.values()) + list(ag_copies.values()):
        for copy in copies:
            copy.wait_send()
    for far, near in finals:
        far.wait()
        near.wait()


def all_reduce(grads_low, grads_top, gains):
    a_rows, a_lanes = grads_low[0].shape
    q_rows, width = grads_low[3].shape
    o_rows = grads_low[4].shape[0]
    half, lanes = a_rows // 2, a_lanes // 2
    b_rows = (o_rows + q_rows) // 12
    shapes_a = [(half, lanes), (half // 2, lanes), (half // 4, lanes)] + [(half // 4, lanes // 2)] * 4
    shapes_b = [(b_rows >> min(step, N_RED), width) for step in range(N_ICI + 1)]
    hbm = pl.BlockSpec(memory_space=pl.ANY)
    vmem = pl.BlockSpec(memory_space=pltpu.VMEM)
    dma = pltpu.SemaphoreType.DMA
    scratch = [pltpu.VMEM((2, 6, half, lanes), F32), pltpu.VMEM((2, 6, b_rows, width), F32)]
    scratch += [pltpu.VMEM((2, 6) + shape, F32) for shape in shapes_a]
    scratch += [pltpu.VMEM((2, 6) + shape, F32) for shape in shapes_b]
    scratch += [pltpu.VMEM((N_ICI + 1,) + gains.shape, F32)]
    scratch += [dma((2, 6, 3)), dma((2, 6, 3)), dma((2, 6, 3)), dma((2, 6, N_ICI, 2)), dma((2, 6, N_ICI, 2)), dma((2, 6, N_RED, 2)), dma((2, 6, N_RED, 2)), dma((2, 6, 3)), dma((2, 6, 3)), dma((2, 6, 3)), dma((N_ICI + 1,)), dma((N_ICI + 1,)), dma]
    return pl.pallas_call(
        functools.partial(all_reduce_kernel, a_rows, a_lanes, q_rows, o_rows),
        in_specs=[hbm] * 10 + [vmem],
        out_specs=[hbm] * 4,
        out_shape=[jax.ShapeDtypeStruct((2, 3, a_rows, a_lanes), F32), jax.ShapeDtypeStruct((2, q_rows, width), F32), jax.ShapeDtypeStruct((2, o_rows, width), F32), jax.ShapeDtypeStruct(gains.shape, F32)],
        scratch_shapes=scratch,
        compiler_params=pltpu.CompilerParams(vmem_limit_bytes=60 * 1024 * 1024, collective_id=0, has_side_effects=True),
        name="all_reduce",
    )(*grads_low, *grads_top, gains)


def dot_c(lhs, rhs, c_l, c_r):
    return lax.dot_general(lhs, rhs, (((c_l,), (c_r,)), ((), ())), preferred_element_type=F32)


def norm_back_t(x_f, inv_rms, gain, d_normed):
    scaled = d_normed * gain
    d_resid = inv_rms * scaled - x_f * (inv_rms ** 3) * jnp.mean(scaled * x_f, axis=0, keepdims=True)
    d_gain = jnp.sum(d_normed * x_f * inv_rms, axis=1)
    return d_resid, d_gain


def layer_forward_t(x_t, weights, cos_t, sin_t, kv_heads, n_group, head_dim):
    g_attn, wqkv_t, w_o, g_ffn, w_gate, w_up, wd_t = weights
    x_f = x_t.astype(F32)
    inv_attn = lax.rsqrt(jnp.mean(x_f * x_f, axis=0, keepdims=True) + NORM_EPS)
    normed = (x_f * inv_attn * g_attn.astype(F32)[:, None]).astype(BF16)
    qkv_t = dot_c(wqkv_t, normed, 1, 0).astype(BF16)
    a_t, rot_t, stats = attn_forward(qkv_t, cos_t, sin_t, kv_heads, n_group, head_dim)
    m_t = (x_f + dot_c(w_o, a_t, 0, 0)).astype(BF16)
    m_f = m_t.astype(F32)
    inv_ffn = lax.rsqrt(jnp.mean(m_f * m_f, axis=0, keepdims=True) + NORM_EPS)
    normed_ffn = (m_f * inv_ffn * g_ffn.astype(F32)[:, None]).astype(BF16)
    gate_t = dot_c(w_gate, normed_ffn, 0, 0).astype(BF16)
    up_t = dot_c(w_up, normed_ffn, 0, 0).astype(BF16)
    return x_f, inv_attn, normed, qkv_t, a_t, rot_t, stats, m_f, inv_ffn, normed_ffn, gate_t, up_t


def layer_backward_t(saved, d_out_t, weights, cos_t, sin_t, kv_heads, n_group, head_dim, scale):
    g_attn, wqkv_t, w_o, g_ffn, w_gate, w_up, wd_t = weights
    x_f, inv_attn, normed, qkv_t, a_t, rot_t, stats, m_f, inv_ffn, normed_ffn, gate_t, up_t = saved
    gate_f = gate_t.astype(F32)
    gate_sig = jax.nn.sigmoid(gate_f)
    silu_act = gate_f * gate_sig
    up_f = up_t.astype(F32)
    hidden = (silu_act * up_f).astype(BF16)
    grad_wd_t = dot_c(d_out_t, hidden, 1, 1) * scale
    d_hidden = dot_c(wd_t, d_out_t, 0, 0).astype(BF16).astype(F32)
    d_gate = (d_hidden * up_f * gate_sig * (1.0 + gate_f * (1.0 - gate_sig))).astype(BF16)
    d_up = (d_hidden * silu_act).astype(BF16)
    grad_w_gate = dot_c(normed_ffn, d_gate, 1, 1) * scale
    grad_w_up = dot_c(normed_ffn, d_up, 1, 1) * scale
    d_normed_ffn = (dot_c(w_gate, d_gate, 1, 0) + dot_c(w_up, d_up, 1, 0)).astype(BF16).astype(F32)
    d_mid_norm, grad_g_ffn = norm_back_t(m_f, inv_ffn, g_ffn.astype(F32)[:, None], d_normed_ffn)
    d_mid = (d_out_t.astype(F32) + d_mid_norm).astype(BF16)
    grad_w_o = dot_c(a_t, d_mid, 1, 1) * scale
    d_attn = dot_c(w_o, d_mid, 1, 0).astype(BF16)
    dqkv_t = attn_backward(rot_t, qkv_t, d_attn, stats, cos_t, sin_t, kv_heads, n_group, head_dim)
    grad_wqkv_t = dot_c(dqkv_t, normed, 1, 1) * scale
    d_normed = dot_c(wqkv_t, dqkv_t, 0, 0).astype(BF16).astype(F32)
    d_x_norm, grad_g_attn = norm_back_t(x_f, inv_attn, g_attn.astype(F32)[:, None], d_normed)
    d_x = (d_mid.astype(F32) + d_x_norm).astype(BF16)
    return d_x, (grad_w_gate, grad_w_up, grad_wd_t, grad_wqkv_t, grad_w_o), (grad_g_attn * scale, grad_g_ffn * scale)


def solution(mesh):
    num_devices = mesh.shape["dp"]
    act_spec = P("dp", None, None)
    rep_spec = P()

    def local_step(x_layer0, x_layer1, d_out, g_attn, w_q, w_k, w_v, w_o, g_ffn, w_gate, w_up, w_down):
        _, seq_len, model_dim = x_layer0.shape
        n_heads, head_dim = w_q.shape[2], w_q.shape[3]
        kv_heads = w_k.shape[2]
        n_group = n_heads // kv_heads
        per = (n_group + 2) * head_dim
        cos_np, sin_np = rope_tables_np(seq_len, head_dim)
        cos_t, sin_t = jnp.asarray(cos_np), jnp.asarray(sin_np)
        scale = 1.0 / num_devices

        def layer_weights(layer):
            def heads_out(w):
                return jnp.transpose(w[layer], (1, 2, 0)).reshape(kv_heads, -1, model_dim)
            wqkv_t = jnp.concatenate([heads_out(w_q), heads_out(w_k), heads_out(w_v)], axis=1).reshape(-1, model_dim)
            return (g_attn[layer], wqkv_t, w_o[layer].reshape(-1, model_dim), g_ffn[layer], w_gate[layer], w_up[layer], jnp.transpose(w_down[layer], (1, 0)))

        x0_t = jnp.transpose(x_layer0[0], (1, 0))
        x1_t = jnp.transpose(x_layer1[0], (1, 0))
        d_top = jnp.transpose(d_out[0], (1, 0))
        w_low, w_top = layer_weights(0), layer_weights(1)
        saved_top = layer_forward_t(x1_t, w_top, cos_t, sin_t, kv_heads, n_group, head_dim)
        d_mid, grads_top, gains_top = layer_backward_t(saved_top, d_top, w_top, cos_t, sin_t, kv_heads, n_group, head_dim, scale)
        saved_low = layer_forward_t(x0_t, w_low, cos_t, sin_t, kv_heads, n_group, head_dim)
        d_x0, grads_low, gains_low = layer_backward_t(saved_low, d_mid, w_low, cos_t, sin_t, kv_heads, n_group, head_dim, scale)
        zero_row = jnp.zeros((model_dim,), F32)
        gains = jnp.stack(gains_low + gains_top + (zero_row,) * 4)
        sum_a, sum_q, sum_o, sum_g = all_reduce(grads_low, grads_top, gains)
        by_group = sum_q.reshape(2, kv_heads, per, model_dim)

        def heads_in(g):
            return jnp.transpose(g.reshape(2, -1, head_dim, model_dim), (0, 3, 1, 2))

        q_end, k_end = n_group * head_dim, (n_group + 1) * head_dim
        d_x = jnp.transpose(d_x0, (1, 0))[None]
        return (d_x, sum_g[0:4:2], heads_in(by_group[:, :, :q_end]), heads_in(by_group[:, :, q_end:k_end]), heads_in(by_group[:, :, k_end:]), sum_o.reshape(2, n_heads, head_dim, model_dim), sum_g[1:4:2], sum_a[:, 0], sum_a[:, 1], jnp.transpose(sum_a[:, 2], (0, 2, 1)))

    return jax.shard_map(local_step, mesh=mesh, in_specs=(act_spec, act_spec, act_spec) + (rep_spec,) * 9, out_specs=(act_spec,) + (rep_spec,) * 9, check_vma=False)
```

```python
import functools

import jax
import jax.numpy as jnp
import numpy as np
from jax import lax
from jax.experimental import pallas as pl
from jax.experimental.pallas import tpu as pltpu
from jax.sharding import PartitionSpec as P

NORM_EPS = 1e-6
ROPE_THETA = 10000.0
BLK = 256
LOG2E = 1.4426950408889634
F32 = jnp.float32
BF16 = jnp.bfloat16


def rope_tables_np(seq_len, head_dim):
    positions = np.arange(seq_len, dtype=np.float32)
    inv_freq = np.float32(ROPE_THETA) ** (-np.arange(0, head_dim, 2, dtype=np.float32) / np.float32(head_dim))
    angles = (positions[None, :] * inv_freq.astype(np.float32)[:, None]).astype(np.float32)
    cos_t = np.repeat(np.cos(angles), 2, axis=0).astype(np.float32)
    sin_t = np.repeat(np.sin(angles), 2, axis=0).astype(np.float32)
    sin_t[0::2] *= -1.0
    return cos_t, sin_t


def pair_swap(values):
    rows = values.shape[0]
    even = lax.broadcasted_iota(jnp.int32, values.shape, 0) % 2 == 0
    return jnp.where(even, pltpu.roll(values, rows - 1, 0), pltpu.roll(values, 1, 0))


def dot_nn(lhs, rhs):
    return lax.dot_general(lhs, rhs, (((1,), (0,)), ((), ())), preferred_element_type=F32)


def dot_nt(lhs, rhs):
    return lax.dot_general(lhs, rhs, (((1,), (1,)), ((), ())), preferred_element_type=F32)


def diag_mask():
    keys = lax.broadcasted_iota(jnp.int32, (BLK, BLK), 0)
    queries = lax.broadcasted_iota(jnp.int32, (BLK, BLK), 1)
    return queries >= keys


def dot_tn(lhs, rhs):
    return lax.dot_general(lhs, rhs, (((0,), (0,)), ((), ())), preferred_element_type=F32)


def ds_of(start, size, align):
    return pl.ds(pl.multiple_of(start, align), size)


def attn_fwd_kernel(att_scale, q_ref, k_ref, v_ref, cos_ref, sin_ref, a_ref, qr_ref, kr_ref, st_ref, k_scr):
    seq_len = q_ref.shape[1]
    n_blk = seq_len // BLK
    cos_t = cos_ref[...]
    sin_t = sin_ref[...]

    @pl.when(pl.program_id(1) == 0)
    def _():
        k_f = k_ref[...].astype(F32)
        k_rot = (k_f * cos_t + pair_swap(k_f) * sin_t).astype(BF16)
        kr_ref[...] = k_rot
        k_scr[...] = k_rot.astype(F32).T.astype(BF16)

    coef = att_scale * LOG2E
    mask = diag_mask()
    q_f = q_ref[...].astype(F32)
    qr_ref[...] = (q_f * cos_t + pair_swap(q_f) * sin_t).astype(BF16)
    st_ref[...] = jnp.zeros_like(st_ref)
    for j in range(n_blk):
        cols = slice(j * BLK, (j + 1) * BLK)
        q_j = qr_ref[:, cols]
        s_blocks = []
        for i in range(j + 1):
            s_i = dot_nn(k_scr[i * BLK:(i + 1) * BLK, :], q_j)
            if i == j:
                s_i = jnp.where(mask, s_i, -1e30)
            s_blocks.append(s_i)
        top = functools.reduce(jnp.maximum, [jnp.max(s_i, axis=0, keepdims=True) for s_i in s_blocks])
        e_blocks = [jnp.exp2((s_i - top) * coef) for s_i in s_blocks]
        total = functools.reduce(jnp.add, [jnp.sum(e_i, axis=0, keepdims=True) for e_i in e_blocks])
        inv = 1.0 / total
        acc = None
        for i in range(j + 1):
            p_i = (e_blocks[i] * inv).astype(BF16)
            part = dot_nn(v_ref[:, i * BLK:(i + 1) * BLK], p_i)
            acc = part if acc is None else acc + part
        a_ref[:, cols] = acc.astype(BF16)
        st_ref[0, 0:1, cols] = top
        st_ref[0, 1:2, cols] = inv


def norm_back_cols(x_f, inv, gain, d_normed):
    scaled = d_normed * gain
    d_resid = inv * scaled - x_f * (inv * inv * inv) * jnp.mean(scaled * x_f, axis=0, keepdims=True)
    return d_resid, d_normed * x_f * inv


def fold_lanes(values):
    return functools.reduce(jnp.add, [values[:, i:i + 128] for i in range(0, values.shape[1], 128)])


def attn_bwd_kernel(att_scale, scale, kv_heads, n_group, qr_ref, kr_ref, v_ref, do_ref, st_ref, cos_ref, sin_ref, x_ref, dmid_ref, gain_ref, w_ref, dx_ref, gw_ref, gg_ref, k_scr, v_scr, dk_acc, dv_acc, dqkv, gacc):
    head_dim, seq_len = qr_ref.shape
    n_blk = seq_len // BLK
    g, h = pl.program_id(0), pl.program_id(1)
    base = g * ((n_group + 2) * head_dim)

    @pl.when(h == 0)
    def _():
        k_scr[...] = kr_ref[...].astype(F32).T.astype(BF16)
        v_scr[...] = v_ref[...].astype(F32).T.astype(BF16)
        dk_acc[...] = jnp.zeros_like(dk_acc)
        dv_acc[...] = jnp.zeros_like(dv_acc)

    coef = att_scale * LOG2E
    mask = diag_mask()
    for j in range(n_blk):
        cols = slice(j * BLK, (j + 1) * BLK)
        q_j = qr_ref[:, cols]
        do_j = do_ref[:, cols]
        top = st_ref[0, 0:1, cols]
        inv = st_ref[0, 1:2, cols]
        p_blocks = []
        dp_blocks = []
        row_dot = None
        for i in range(j + 1):
            keys = slice(i * BLK, (i + 1) * BLK)
            s_i = dot_nn(k_scr[keys, :], q_j)
            if i == j:
                s_i = jnp.where(mask, s_i, -1e30)
            p_i = jnp.exp2((s_i - top) * coef) * inv
            dp_i = dot_nn(v_scr[keys, :], do_j).astype(BF16).astype(F32)
            part = jnp.sum(p_i * dp_i, axis=0, keepdims=True)
            row_dot = part if row_dot is None else row_dot + part
            dv_acc[:, keys] += dot_nt(do_j, p_i.astype(BF16))
            p_blocks.append(p_i)
            dp_blocks.append(dp_i)
        dq_j = None
        for i in range(j + 1):
            keys = slice(i * BLK, (i + 1) * BLK)
            ds_i = (p_blocks[i] * (dp_blocks[i] - row_dot) * att_scale).astype(BF16)
            part = dot_nn(kr_ref[:, keys], ds_i)
            dq_j = part if dq_j is None else dq_j + part
            dk_acc[:, keys] += dot_nt(q_j, ds_i)
        dq_j = dq_j.astype(BF16).astype(F32)
        dqkv[ds_of(base + h * head_dim, head_dim, head_dim), cols] = (dq_j * cos_ref[:, cols] - pair_swap(dq_j) * sin_ref[:, cols]).astype(BF16)

    @pl.when(h == n_group - 1)
    def _():
        d_k = dk_acc[...].astype(BF16).astype(F32)
        dqkv[ds_of(base + n_group * head_dim, head_dim, head_dim), :] = (d_k * cos_ref[...] - pair_swap(d_k) * sin_ref[...]).astype(BF16)
        dqkv[ds_of(base + (n_group + 1) * head_dim, head_dim, head_dim), :] = dv_acc[...].astype(BF16)

    @pl.when((g == kv_heads - 1) & (h == n_group - 1))
    def _():
        gacc[...] = jnp.zeros_like(gacc)
        gw_ref[...] = jnp.zeros_like(gw_ref)
        gain = gain_ref[...]

        @pl.loop(0, n_blk)
        def _(j):
            cols = ds_of(j * BLK, BLK, BLK)
            x_f = x_ref[:, cols].astype(F32)
            inv = lax.rsqrt(jnp.mean(x_f * x_f, axis=0, keepdims=True) + NORM_EPS)
            normed = (x_f * inv * gain).astype(BF16)
            gw_ref[...] += dot_nt(dqkv[:, cols], normed)
            d_normed = dot_tn(w_ref[...], dqkv[:, cols]).astype(BF16).astype(F32)
            d_resid, d_gain = norm_back_cols(x_f, inv, gain, d_normed)
            gacc[...] += fold_lanes(d_gain)
            dx_ref[:, cols] = (dmid_ref[:, cols].astype(F32) + d_resid).astype(BF16)

        gw_ref[...] = gw_ref[...] * scale
        gg_ref[...] = jnp.sum(gacc[...], axis=1, keepdims=True) * scale


def ffn_kernel(scale, x_ref, a_ref, dout_ref, wo_ref, gain_ref, wg_ref, wu_ref, wd_ref, dmid_ref, dattn_ref, gwo_ref, gg_ref, gwg_ref, gwu_ref, gwd_ref, m_scr, n_scr, inv_scr, acc, hid, dg, du, gacc):
    model_dim, seq_len = x_ref.shape
    n_blk = seq_len // BLK
    step = pl.program_id(0)
    gain = gain_ref[...]

    @pl.when(step == 0)
    def _():
        @pl.loop(0, n_blk)
        def _(j):
            cols = ds_of(j * BLK, BLK, BLK)
            m_b = (x_ref[:, cols].astype(F32) + dot_tn(wo_ref[...], a_ref[:, cols])).astype(BF16)
            m_scr[:, cols] = m_b
            m_f = m_b.astype(F32)
            inv = lax.rsqrt(jnp.mean(m_f * m_f, axis=0, keepdims=True) + NORM_EPS)
            inv_scr[0:1, cols] = inv
            n_scr[:, cols] = (m_f * inv * gain).astype(BF16)
        acc[...] = jnp.zeros_like(acc)
        gacc[...] = jnp.zeros_like(gacc)

    w_g = wg_ref[...]
    w_u = wu_ref[...]
    for j in range(n_blk):
        cols = slice(j * BLK, (j + 1) * BLK)
        gate_f = dot_tn(w_g, n_scr[:, cols]).astype(BF16).astype(F32)
        up_f = dot_tn(w_u, n_scr[:, cols]).astype(BF16).astype(F32)
        d_hidden = dot_tn(wd_ref[...], dout_ref[:, cols]).astype(BF16).astype(F32)
        gate_sig = jax.nn.sigmoid(gate_f)
        silu_act = gate_f * gate_sig
        hid[:, cols] = (silu_act * up_f).astype(BF16)
        dg[:, cols] = (d_hidden * up_f * gate_sig * (1.0 + gate_f * (1.0 - gate_sig))).astype(BF16)
        du[:, cols] = (d_hidden * silu_act).astype(BF16)
        acc[:, cols] += dot_nn(w_g, dg[:, cols]) + dot_nn(w_u, du[:, cols])
    gwg_ref[...] = dot_nt(n_scr[...], dg[...]) * scale
    gwu_ref[...] = dot_nt(n_scr[...], du[...]) * scale
    gwd_ref[...] = dot_nt(dout_ref[...], hid[...]) * scale

    @pl.when(step == pl.num_programs(0) - 1)
    def _():
        gwo_ref[...] = jnp.zeros_like(gwo_ref)

        @pl.loop(0, n_blk)
        def _(j):
            cols = ds_of(j * BLK, BLK, BLK)
            d_normed = acc[:, cols].astype(BF16).astype(F32)
            d_resid, d_gain = norm_back_cols(m_scr[:, cols].astype(F32), inv_scr[0:1, cols], gain, d_normed)
            gacc[...] += fold_lanes(d_gain)
            d_mid = (dout_ref[:, cols].astype(F32) + d_resid).astype(BF16)
            dmid_ref[:, cols] = d_mid
            dattn_ref[:, cols] = dot_nn(wo_ref[...], d_mid).astype(BF16)
            gwo_ref[...] += dot_nt(a_ref[:, cols], d_mid)

        gwo_ref[...] = gwo_ref[...] * scale
        gg_ref[...] = jnp.sum(gacc[...], axis=1, keepdims=True) * scale


def whole(shape):
    return pl.BlockSpec(shape, lambda *_: (0,) * len(shape))


def attn_forward(qkv_t, cos_t, sin_t, kv_heads, n_group, head_dim):
    seq_len = qkv_t.shape[1]
    per = n_group + 2
    block = (head_dim, seq_len)
    flops = 2 * 2 * kv_heads * n_group * head_dim * seq_len * seq_len
    return pl.pallas_call(
        functools.partial(attn_fwd_kernel, head_dim ** -0.5),
        grid=(kv_heads, n_group),
        in_specs=[pl.BlockSpec(block, lambda g, h: (g * per + h, 0)), pl.BlockSpec(block, lambda g, h: (g * per + n_group, 0)), pl.BlockSpec(block, lambda g, h: (g * per + n_group + 1, 0)), whole(block), whole(block)],
        out_specs=[pl.BlockSpec(block, lambda g, h: (g * n_group + h, 0)), pl.BlockSpec(block, lambda g, h: (g * n_group + h, 0)), pl.BlockSpec(block, lambda g, h: (g, 0)), pl.BlockSpec((1, 8, seq_len), lambda g, h: (g * n_group + h, 0, 0))],
        out_shape=[jax.ShapeDtypeStruct((kv_heads * n_group * head_dim, seq_len), BF16), jax.ShapeDtypeStruct((kv_heads * n_group * head_dim, seq_len), BF16), jax.ShapeDtypeStruct((kv_heads * head_dim, seq_len), BF16), jax.ShapeDtypeStruct((kv_heads * n_group, 8, seq_len), F32)],
        scratch_shapes=[pltpu.VMEM((seq_len, head_dim), BF16)],
        compiler_params=pltpu.CompilerParams(vmem_limit_bytes=40 * 1024 * 1024),
        cost_estimate=pl.CostEstimate(flops=8 * flops, bytes_accessed=8 * qkv_t.size, transcendentals=0),
        name="attn_fwd",
    )(qkv_t, qkv_t, qkv_t, cos_t, sin_t)


def attn_backward(qr_t, kr_t, qkv_t, do_t, stats, cos_t, sin_t, x_t, d_mid, gain, wqkv_t, scale, kv_heads, n_group, head_dim):
    model_dim, seq_len = x_t.shape
    per = n_group + 2
    block = (head_dim, seq_len)
    flops = 5 * 2 * kv_heads * n_group * head_dim * seq_len * seq_len
    return pl.pallas_call(
        functools.partial(attn_bwd_kernel, head_dim ** -0.5, scale, kv_heads, n_group),
        grid=(kv_heads, n_group),
        in_specs=[
            pl.BlockSpec(block, lambda g, h: (g * n_group + h, 0)),
            pl.BlockSpec(block, lambda g, h: (g, 0)),
            pl.BlockSpec(block, lambda g, h: (g * per + n_group + 1, 0)),
            pl.BlockSpec(block, lambda g, h: (g * n_group + h, 0)),
            pl.BlockSpec((1, 8, seq_len), lambda g, h: (g * n_group + h, 0, 0)),
            whole(block),
            whole(block),
            whole(x_t.shape),
            whole(x_t.shape),
            whole((model_dim, 1)),
            whole(wqkv_t.shape),
        ],
        out_specs=[whole(x_t.shape), whole(wqkv_t.shape), whole((model_dim, 1))],
        out_shape=[jax.ShapeDtypeStruct(x_t.shape, BF16), jax.ShapeDtypeStruct(wqkv_t.shape, F32), jax.ShapeDtypeStruct((model_dim, 1), F32)],
        scratch_shapes=[pltpu.VMEM((seq_len, head_dim), BF16), pltpu.VMEM((seq_len, head_dim), BF16), pltpu.VMEM(block, F32), pltpu.VMEM(block, F32), pltpu.VMEM(qkv_t.shape, BF16), pltpu.VMEM((model_dim, 128), F32)],
        compiler_params=pltpu.CompilerParams(vmem_limit_bytes=50 * 1024 * 1024),
        cost_estimate=pl.CostEstimate(flops=8 * flops, bytes_accessed=8 * qkv_t.size, transcendentals=0),
        name="attn_bwd",
    )(qr_t, kr_t, qkv_t, do_t, stats, cos_t, sin_t, x_t, d_mid, gain, wqkv_t)


def ffn(x_t, a_t, d_out_t, w_o, gain, w_gate, w_up, wd_t, scale):
    model_dim, seq_len = x_t.shape
    ff_dim = w_gate.shape[1]
    w_spec = pl.BlockSpec((model_dim, BLK), lambda f: (0, f))
    act = jax.ShapeDtypeStruct(x_t.shape, BF16)
    grad = jax.ShapeDtypeStruct(w_gate.shape, F32)
    return pl.pallas_call(
        functools.partial(ffn_kernel, scale),
        grid=(ff_dim // BLK,),
        in_specs=[whole(x_t.shape), whole(a_t.shape), whole(x_t.shape), whole(w_o.shape), whole((model_dim, 1)), w_spec, w_spec, w_spec],
        out_specs=[whole(x_t.shape), whole(a_t.shape), whole(w_o.shape), whole((model_dim, 1)), w_spec, w_spec, w_spec],
        out_shape=[act, jax.ShapeDtypeStruct(a_t.shape, BF16), jax.ShapeDtypeStruct(w_o.shape, F32), jax.ShapeDtypeStruct((model_dim, 1), F32), grad, grad, grad],
        scratch_shapes=[pltpu.VMEM(x_t.shape, BF16), pltpu.VMEM(x_t.shape, BF16), pltpu.VMEM((8, seq_len), F32), pltpu.VMEM(x_t.shape, F32), pltpu.VMEM((BLK, seq_len), BF16), pltpu.VMEM((BLK, seq_len), BF16), pltpu.VMEM((BLK, seq_len), BF16), pltpu.VMEM((model_dim, 128), F32)],
        compiler_params=pltpu.CompilerParams(vmem_limit_bytes=55 * 1024 * 1024),
        cost_estimate=pl.CostEstimate(flops=18 * x_t.size * ff_dim, bytes_accessed=20 * w_gate.size, transcendentals=0),
        name="ffn",
    )(x_t, a_t, d_out_t, w_o, gain, w_gate, w_up, wd_t)


MESH = pl.DeviceIdType.MESH
N_RED = 3
N_ICI = 6


def add_rows(dst, src, rows, step):
    @pl.loop(0, rows // step)
    def _(i):
        part = pl.ds(pl.multiple_of(i * step, 8), step)
        dst[part, :] = dst[part, :] + src[part, :]


def all_reduce_kernel(a_rows, a_lanes, q_rows, o_rows, *refs):
    srcs = [refs[5 * layer:5 * layer + 5] for layer in range(2)]
    gain_ref = refs[10]
    outs_a = refs[11:14]
    out_q, out_o, out_g = refs[14:17]
    acc_a, acc_b = refs[17:19]
    bufs_a = refs[19:26]
    bufs_b = refs[26:33]
    gain_bufs = refs[33]
    (core_send, core_recv, load_sem, ici_send, ici_recv, ag_send, ag_recv, fin_send, fin_recv, fin_loc, g_send, g_recv, g_loc) = refs[34:47]

    me = lax.axis_index("dp")
    core = lax.rem(me, 2)
    coords = (lax.rem(me // 2, 4), lax.rem(me // 8, 4), me // 32)
    strides = (2, 8, 32)
    peer = me + 1 - 2 * core
    gens = []
    for kind in range(2):
        for axis in range(3):
            v = coords[axis]
            if kind == 0:
                partner, bit = v + 1 - 2 * lax.rem(v, 2), lax.rem(v + v // 2, 2)
            else:
                partner, bit = 3 - v, v // 2
            gens.append((me + (partner - v) * strides[axis], bit))

    barrier = pltpu.get_barrier_semaphore()
    for dev in [peer] + [g[0] for g in gens]:
        pl.semaphore_signal(barrier, inc=1, device_id=(dev,), device_id_type=MESH)
    pl.semaphore_wait(barrier, 1 + N_ICI)

    half = a_rows // 2
    lanes = a_lanes // 2
    o_half = o_rows // 12
    q_half = q_rows // 12
    b_rows = o_half + q_half

    def ds8(start, size):
        return pl.ds(pl.multiple_of(start, 8), size)

    def remote(src, dst, send, recv, dev):
        return pltpu.make_async_remote_copy(src_ref=src, dst_ref=dst, send_sem=send, recv_sem=recv, device_id=(dev,), device_id_type=MESH)

    flows = [(layer, k) for layer in (1, 0) for k in range(6)]
    core_copies = {}
    load_copies = {}
    for layer, k in flows:
        mat = srcs[layer][k // 2]
        q_src, o_src = srcs[layer][3:]
        lane = slice((k % 2) * lanes, (k % 2 + 1) * lanes)

        def parts(which):
            return (
                (mat.at[ds8(which * half, half), lane], lambda buf_a, buf_b: buf_a.at[layer, k]),
                (o_src.at[ds8(k * 2 * o_half + which * o_half, o_half), :], lambda buf_a, buf_b: buf_b.at[layer, k, 0:o_half, :]),
                (q_src.at[ds8(k * 2 * q_half + which * q_half, q_half), :], lambda buf_a, buf_b: buf_b.at[layer, k, o_half:b_rows, :]),
            )

        sends = [remote(src, dst(bufs_a[0], bufs_b[0]), core_send.at[layer, k, p], core_recv.at[layer, k, p], peer) for p, (src, dst) in enumerate(parts(1 - core))]
        loads = [pltpu.make_async_copy(src, dst(acc_a, acc_b), load_sem.at[layer, k, p]) for p, (src, dst) in enumerate(parts(core))]
        for copy in sends + loads:
            copy.start()
        core_copies[layer, k] = sends
        load_copies[layer, k] = loads
    gain_copy = remote(gain_ref, gain_bufs.at[0], g_send.at[0], g_recv.at[0], peer)
    gain_copy.start()

    def part_a(step, buf, bit_keep):
        if step == 0:
            return buf.at[ds8(bit_keep * (half // 2), half // 2), :]
        if step == 1:
            return buf.at[ds8(bit_keep * (half // 4), half // 4), :]
        return buf.at[:, pl.ds(pl.multiple_of(bit_keep * (lanes // 2), 128), lanes // 2)]

    def part_b(step, buf, bit_keep):
        size = b_rows >> (step + 1)
        return buf.at[ds8(bit_keep * size, size), :]

    a_size = [half, half // 2, half // 4] + [half // 4] * 4
    b_size = [b_rows >> min(step, N_RED) for step in range(N_ICI + 1)]
    a_step = 24
    ici_copies = {}
    pending = []

    def flush():
        while pending:
            for copy in pending.pop(0):
                copy.start()

    for step in range(N_ICI + 1):
        for layer, k in flows:
            cur_a, cur_b = bufs_a[step].at[layer, k], bufs_b[step].at[layer, k]
            if step == 0:
                for copy in load_copies[layer, k]:
                    copy.wait()
                for copy in core_copies[layer, k]:
                    copy.wait_recv()
                old_a, old_b = acc_a.at[layer, k], acc_b.at[layer, k]
            else:
                for copy in ici_copies[layer, k, step - 1]:
                    copy.wait_recv()
                old_a, old_b = bufs_a[step - 1].at[layer, k], bufs_b[step - 1].at[layer, k]
                if step <= N_RED:
                    bit = gens[(k + step - 1) % N_ICI][1]
                    old_a, old_b = part_a(step - 1, old_a, bit), part_b(step - 1, old_b, bit)
            add_rows(cur_a, old_a, a_size[step], a_step)
            add_rows(cur_b, old_b, b_size[step], 16)
            if step < N_ICI:
                dev, bit = gens[(k + step) % N_ICI]
                src_a, src_b = cur_a, cur_b
                if step < N_RED:
                    src_a, src_b = part_a(step, cur_a, 1 - bit), part_b(step, cur_b, 1 - bit)
                copies = [
                    remote(src_a, bufs_a[step + 1].at[layer, k], ici_send.at[layer, k, step, 0], ici_recv.at[layer, k, step, 0], dev),
                    remote(src_b, bufs_b[step + 1].at[layer, k], ici_send.at[layer, k, step, 1], ici_recv.at[layer, k, step, 1], dev),
                ]
                ici_copies[layer, k, step] = copies
                flush()
                pending.append(copies)
        flush()
        gain_copy.wait()
        gain_old = gain_ref if step == 0 else gain_bufs.at[step - 1]
        gain_bufs[step, :, :] = gain_bufs[step, :, :] + gain_old[...]
        if step < N_ICI:
            gain_copy = remote(gain_bufs.at[step], gain_bufs.at[step + 1], g_send.at[step + 1], g_recv.at[step + 1], gens[step][0])
            gain_copy.start()
    gain_out = pltpu.make_async_copy(gain_bufs.at[N_ICI], out_g, g_loc)
    gain_out.start()

    def ag_region(layer, k, step):
        bits = [gens[(k + s) % N_ICI][1] for s in range(N_RED)]
        a_off = sum([bits[s] * (half >> (s + 1)) for s in range(min(step, 1) + 1)])
        b_off = sum([bits[s] * (b_rows >> (s + 1)) for s in range(step + 1)])
        a_cnt = half >> (min(step, 1) + 1)
        view_a = acc_a.at[layer, k, ds8(a_off, a_cnt), :]
        if step == 2:
            view_a = acc_a.at[layer, k, ds8(a_off, a_cnt), pl.ds(pl.multiple_of(bits[2] * (lanes // 2), 128), lanes // 2)]
        return view_a, acc_b.at[layer, k, ds8(b_off, b_rows >> (step + 1)), :]

    ag_copies = {}
    for step in reversed(range(N_RED)):
        for layer, k in flows:
            view_a, view_b = ag_region(layer, k, step)
            if step == N_RED - 1:
                last_a, last_b = bufs_a[N_ICI], bufs_b[N_ICI]
                view_a[...] = last_a[layer, k, :, :]
                view_b[...] = last_b[layer, k, :, :]
            else:
                for copy in ag_copies[layer, k, step + 1]:
                    copy.wait_recv()
            dev = gens[(k + step) % N_ICI][0]
            copies = [
                remote(view_a, view_a, ag_send.at[layer, k, step, 0], ag_recv.at[layer, k, step, 0], dev),
                remote(view_b, view_b, ag_send.at[layer, k, step, 1], ag_recv.at[layer, k, step, 1], dev),
            ]
            ag_copies[layer, k, step] = copies
            flush()
            pending.append(copies)
        flush()

    finals = []
    for layer, k in flows:
        for copy in ag_copies[layer, k, 0]:
            copy.wait_recv()
        lane = slice((k % 2) * lanes, (k % 2 + 1) * lanes)
        moves = [
            (acc_a.at[layer, k], outs_a[k // 2].at[layer, ds8(core * half, half), lane]),
            (acc_b.at[layer, k, 0:o_half, :], out_o.at[layer, ds8(k * 2 * o_half + core * o_half, o_half), :]),
            (acc_b.at[layer, k, o_half:b_rows, :], out_q.at[layer, ds8(k * 2 * q_half + core * q_half, q_half), :]),
        ]
        for p, (src, dst) in enumerate(moves):
            far = remote(src, dst, fin_send.at[layer, k, p], fin_recv.at[layer, k, p], peer)
            near = pltpu.make_async_copy(src, dst, fin_loc.at[layer, k, p])
            far.start()
            near.start()
            finals.append((far, near))
    gain_out.wait()
    for copies in core_copies.values():
        for copy in copies:
            copy.wait_send()
    for copies in list(ici_copies.values()) + list(ag_copies.values()):
        for copy in copies:
            copy.wait_send()
    for far, near in finals:
        far.wait()
        near.wait()


def all_reduce(grads_low, grads_top, gains):
    a_rows, a_lanes = grads_low[0].shape
    q_rows, width = grads_low[3].shape
    o_rows = grads_low[4].shape[0]
    half, lanes = a_rows // 2, a_lanes // 2
    b_rows = (o_rows + q_rows) // 12
    shapes_a = [(half, lanes), (half // 2, lanes), (half // 4, lanes)] + [(half // 4, lanes // 2)] * 4
    shapes_b = [(b_rows >> min(step, N_RED), width) for step in range(N_ICI + 1)]
    hbm = pl.BlockSpec(memory_space=pl.ANY)
    vmem = pl.BlockSpec(memory_space=pltpu.VMEM)
    dma = pltpu.SemaphoreType.DMA
    scratch = [pltpu.VMEM((2, 6, half, lanes), F32), pltpu.VMEM((2, 6, b_rows, width), F32)]
    scratch += [pltpu.VMEM((2, 6) + shape, F32) for shape in shapes_a]
    scratch += [pltpu.VMEM((2, 6) + shape, F32) for shape in shapes_b]
    scratch += [pltpu.VMEM((N_ICI + 1,) + gains.shape, F32)]
    scratch += [dma((2, 6, 3)), dma((2, 6, 3)), dma((2, 6, 3)), dma((2, 6, N_ICI, 2)), dma((2, 6, N_ICI, 2)), dma((2, 6, N_RED, 2)), dma((2, 6, N_RED, 2)), dma((2, 6, 3)), dma((2, 6, 3)), dma((2, 6, 3)), dma((N_ICI + 1,)), dma((N_ICI + 1,)), dma]
    return pl.pallas_call(
        functools.partial(all_reduce_kernel, a_rows, a_lanes, q_rows, o_rows),
        in_specs=[hbm] * 10 + [vmem],
        out_specs=[hbm] * 6,
        out_shape=[jax.ShapeDtypeStruct((2, a_rows, a_lanes), F32)] * 3 + [jax.ShapeDtypeStruct((2, q_rows, width), F32), jax.ShapeDtypeStruct((2, o_rows, width), F32), jax.ShapeDtypeStruct(gains.shape, F32)],
        scratch_shapes=scratch,
        compiler_params=pltpu.CompilerParams(vmem_limit_bytes=60 * 1024 * 1024, collective_id=0, has_side_effects=True),
        name="all_reduce",
    )(*grads_low, *grads_top, gains)


def layer_qkv(x_t, weights):
    x_f = x_t.astype(F32)
    inv_attn = lax.rsqrt(jnp.mean(x_f * x_f, axis=0, keepdims=True) + NORM_EPS)
    normed = (x_f * inv_attn * weights[0]).astype(BF16)
    return lax.dot_general(weights[1], normed, (((1,), (0,)), ((), ())), preferred_element_type=F32).astype(BF16)


def layer_backward(x_t, d_out_t, weights, cos_t, sin_t, scale, dims):
    g_attn, wqkv_t, w_o, g_ffn, w_gate, w_up, wd_t = weights
    qkv_t = layer_qkv(x_t, weights)
    a_t, qr_t, kr_t, stats = attn_forward(qkv_t, cos_t, sin_t, *dims)
    d_mid, d_attn, grad_w_o, grad_g_ffn, grad_w_gate, grad_w_up, grad_wd_t = ffn(x_t, a_t, d_out_t, w_o, g_ffn, w_gate, w_up, wd_t, scale)
    d_x, grad_wqkv_t, grad_g_attn = attn_backward(qr_t, kr_t, qkv_t, d_attn, stats, cos_t, sin_t, x_t, d_mid, g_attn, wqkv_t, scale, *dims)
    return d_x, (grad_w_gate, grad_w_up, grad_wd_t, grad_wqkv_t, grad_w_o), (grad_g_attn[:, 0], grad_g_ffn[:, 0])


def solution(mesh):
    num_devices = mesh.shape["dp"]
    act_spec = P("dp", None, None)
    rep_spec = P()

    def local_step(x_layer0, x_layer1, d_out, g_attn, w_q, w_k, w_v, w_o, g_ffn, w_gate, w_up, w_down):
        _, seq_len, model_dim = x_layer0.shape
        n_heads, head_dim = w_q.shape[2], w_q.shape[3]
        kv_heads = w_k.shape[2]
        n_group = n_heads // kv_heads
        per = (n_group + 2) * head_dim
        cos_np, sin_np = rope_tables_np(seq_len, head_dim)
        cos_t, sin_t = jnp.asarray(cos_np), jnp.asarray(sin_np)
        scale = 1.0 / num_devices

        def layer_weights(layer):
            def heads_out(w):
                return jnp.transpose(w[layer], (1, 2, 0)).reshape(kv_heads, -1, model_dim)
            wqkv_t = jnp.concatenate([heads_out(w_q), heads_out(w_k), heads_out(w_v)], axis=1).reshape(-1, model_dim)
            return (g_attn[layer].astype(F32)[:, None], wqkv_t, w_o[layer].reshape(-1, model_dim), g_ffn[layer].astype(F32)[:, None], w_gate[layer], w_up[layer], jnp.transpose(w_down[layer], (1, 0)))

        x0_t = jnp.transpose(x_layer0[0], (1, 0))
        x1_t = jnp.transpose(x_layer1[0], (1, 0))
        d_top = jnp.transpose(d_out[0], (1, 0))
        w_low, w_top = layer_weights(0), layer_weights(1)
        dims = (kv_heads, n_group, head_dim)
        d_mid, grads_top, gains_top = layer_backward(x1_t, d_top, w_top, cos_t, sin_t, scale, dims)
        d_x0, grads_low, gains_low = layer_backward(x0_t, d_mid, w_low, cos_t, sin_t, scale, dims)
        zero_row = jnp.zeros((model_dim,), F32)
        gains = jnp.stack(gains_low + gains_top + (zero_row,) * 4)
        sum_gate, sum_up, sum_wd, sum_q, sum_o, sum_g = all_reduce(grads_low, grads_top, gains)
        by_group = sum_q.reshape(2, kv_heads, per, model_dim)

        def heads_in(g):
            return jnp.transpose(g.reshape(2, -1, head_dim, model_dim), (0, 3, 1, 2))

        q_end, k_end = n_group * head_dim, (n_group + 1) * head_dim
        d_x = jnp.transpose(d_x0, (1, 0))[None]
        return (d_x, sum_g[0:4:2], heads_in(by_group[:, :, :q_end]), heads_in(by_group[:, :, q_end:k_end]), heads_in(by_group[:, :, k_end:]), sum_o.reshape(2, n_heads, head_dim, model_dim), sum_g[1:4:2], sum_gate, sum_up, jnp.transpose(sum_wd, (0, 2, 1)))

    return jax.shard_map(local_step, mesh=mesh, in_specs=(act_spec, act_spec, act_spec) + (rep_spec,) * 9, out_specs=(act_spec,) + (rep_spec,) * 9, check_vma=False)
```

```python
import functools

import jax
import jax.numpy as jnp
import numpy as np
from jax import lax
from jax.experimental import pallas as pl
from jax.experimental.pallas import tpu as pltpu
from jax.sharding import PartitionSpec as P

NORM_EPS = 1e-6
ROPE_THETA = 10000.0
BLK = 256
LOG2E = 1.4426950408889634
F32 = jnp.float32
BF16 = jnp.bfloat16


def rope_tables_np(seq_len, head_dim):
    positions = np.arange(seq_len, dtype=np.float32)
    inv_freq = np.float32(ROPE_THETA) ** (-np.arange(0, head_dim, 2, dtype=np.float32) / np.float32(head_dim))
    angles = (positions[None, :] * inv_freq.astype(np.float32)[:, None]).astype(np.float32)
    cos_t = np.repeat(np.cos(angles), 2, axis=0).astype(np.float32)
    sin_t = np.repeat(np.sin(angles), 2, axis=0).astype(np.float32)
    sin_t[0::2] *= -1.0
    return cos_t, sin_t


def pair_swap(values):
    rows = values.shape[0]
    even = lax.broadcasted_iota(jnp.int32, values.shape, 0) % 2 == 0
    return jnp.where(even, pltpu.roll(values, rows - 1, 0), pltpu.roll(values, 1, 0))


def dot_nn(lhs, rhs):
    return lax.dot_general(lhs, rhs, (((1,), (0,)), ((), ())), preferred_element_type=F32)


def dot_nt(lhs, rhs):
    return lax.dot_general(lhs, rhs, (((1,), (1,)), ((), ())), preferred_element_type=F32)


def diag_mask():
    keys = lax.broadcasted_iota(jnp.int32, (BLK, BLK), 0)
    queries = lax.broadcasted_iota(jnp.int32, (BLK, BLK), 1)
    return queries >= keys


def dot_tn(lhs, rhs):
    return lax.dot_general(lhs, rhs, (((0,), (0,)), ((), ())), preferred_element_type=F32)


def ds_of(start, size, align):
    return pl.ds(pl.multiple_of(start, align), size)


def norm_back_cols(x_f, inv, gain, d_normed):
    scaled = d_normed * gain
    d_resid = inv * scaled - x_f * (inv * inv * inv) * jnp.mean(scaled * x_f, axis=0, keepdims=True)
    return d_resid, d_normed * x_f * inv


def fold_lanes(values):
    return functools.reduce(jnp.add, [values[:, i:i + 128] for i in range(0, values.shape[1], 128)])


MESH = pl.DeviceIdType.MESH
N_RED = 3
N_ICI = 6
FLOWS = range(6)


def ds8(start, size):
    return pl.ds(pl.multiple_of(start, 8), size)


def remote(src, dst, send, recv, dev):
    return pltpu.make_async_remote_copy(src_ref=src, dst_ref=dst, send_sem=send, recv_sem=recv, device_id=(dev,), device_id_type=MESH)


def add_rows(dst, src, rows, step):
    @pl.loop(0, rows // step)
    def _(i):
        part = pl.ds(pl.multiple_of(i * step, 8), step)
        dst[part, :] = dst[part, :] + src[part, :]


class Comm:
    def __init__(self, dims, srcs, outs, refs):
        a_rows, a_lanes, q_rows, o_rows = dims
        self.srcs, self.outs = srcs, outs
        self.acc_a, self.acc_b = refs[0:2]
        self.bufs_a, self.bufs_b = refs[2:9], refs[9:16]
        (self.core_send, self.core_recv, self.load_sem, self.ici_send, self.ici_recv, self.ag_send, self.ag_recv, self.fin_send, self.fin_recv, self.fin_loc) = refs[16:26]
        self.half, self.lanes = a_rows // 2, a_lanes // 2
        self.o_half, self.q_half = o_rows // 12, q_rows // 12
        self.b_rows = self.o_half + self.q_half
        me = lax.axis_index("dp")
        self.core = lax.rem(me, 2)
        coords = (lax.rem(me // 2, 4), lax.rem(me // 8, 4), me // 32)
        strides = (2, 8, 32)
        self.peer = me + 1 - 2 * self.core
        self.gens = []
        for kind in range(2):
            for axis in range(3):
                v = coords[axis]
                if kind == 0:
                    partner, bit = v + 1 - 2 * lax.rem(v, 2), lax.rem(v + v // 2, 2)
                else:
                    partner, bit = 3 - v, v // 2
                self.gens.append((me + (partner - v) * strides[axis], bit))

    def barrier(self):
        barrier = pltpu.get_barrier_semaphore()
        for dev in [self.peer] + [g[0] for g in self.gens]:
            pl.semaphore_signal(barrier, inc=1, device_id=(dev,), device_id_type=MESH)
        pl.semaphore_wait(barrier, 1 + N_ICI)

    def gen(self, k, step):
        return self.gens[(k + step) % N_ICI]

    def core_parts(self, k, which, buf_a, buf_b):
        lane = slice((k % 2) * self.lanes, (k % 2 + 1) * self.lanes)
        q_src, o_src = self.srcs[3:]
        o_half, q_half = self.o_half, self.q_half
        return (
            (self.srcs[k // 2].at[ds8(which * self.half, self.half), lane], buf_a.at[k]),
            (o_src.at[ds8(k * 2 * o_half + which * o_half, o_half), :], buf_b.at[k, 0:o_half, :]),
            (q_src.at[ds8(k * 2 * q_half + which * q_half, q_half), :], buf_b.at[k, o_half:self.b_rows, :]),
        )

    def core_sends(self, k):
        return [remote(src, dst, self.core_send.at[k, p], self.core_recv.at[k, p], self.peer) for p, (src, dst) in enumerate(self.core_parts(k, 1 - self.core, self.bufs_a[0], self.bufs_b[0]))]

    def core_loads(self, k):
        return [pltpu.make_async_copy(src, dst, self.load_sem.at[k, p]) for p, (src, dst) in enumerate(self.core_parts(k, self.core, self.acc_a, self.acc_b))]

    def open(self):
        for k in FLOWS:
            for copy in self.core_sends(k) + self.core_loads(k):
                copy.start()

    def part_a(self, step, buf, bit):
        if step < 2:
            size = self.half >> (step + 1)
            return buf.at[ds8(bit * size, size), :]
        return buf.at[:, pl.ds(pl.multiple_of(bit * (self.lanes // 2), 128), self.lanes // 2)]

    def part_b(self, step, buf, bit):
        size = self.b_rows >> (step + 1)
        return buf.at[ds8(bit * size, size), :]

    def ici(self, k, step):
        dev, bit = self.gen(k, step)
        src_a, src_b = self.bufs_a[step].at[k], self.bufs_b[step].at[k]
        if step < N_RED:
            src_a, src_b = self.part_a(step, src_a, 1 - bit), self.part_b(step, src_b, 1 - bit)
        return [
            remote(src_a, self.bufs_a[step + 1].at[k], self.ici_send.at[k, step, 0], self.ici_recv.at[k, step, 0], dev),
            remote(src_b, self.bufs_b[step + 1].at[k], self.ici_send.at[k, step, 1], self.ici_recv.at[k, step, 1], dev),
        ]

    def ag_region(self, k, step):
        bits = [self.gen(k, s)[1] for s in range(N_RED)]
        a_off = sum([bits[s] * (self.half >> (s + 1)) for s in range(min(step, 1) + 1)])
        b_off = sum([bits[s] * (self.b_rows >> (s + 1)) for s in range(step + 1)])
        rows_a = ds8(a_off, self.half >> (min(step, 1) + 1))
        if step == 2:
            view_a = self.acc_a.at[k, rows_a, pl.ds(pl.multiple_of(bits[2] * (self.lanes // 2), 128), self.lanes // 2)]
        else:
            view_a = self.acc_a.at[k, rows_a, :]
        return view_a, self.acc_b.at[k, ds8(b_off, self.b_rows >> (step + 1)), :]

    def ag(self, k, step):
        dev = self.gen(k, step)[0]
        return [remote(view, view, self.ag_send.at[k, step, p], self.ag_recv.at[k, step, p], dev) for p, view in enumerate(self.ag_region(k, step))]

    def final(self, k):
        lane = slice((k % 2) * self.lanes, (k % 2 + 1) * self.lanes)
        out_q, out_o = self.outs[3:]
        o_half, q_half = self.o_half, self.q_half
        moves = (
            (self.acc_a.at[k], self.outs[k // 2].at[ds8(self.core * self.half, self.half), lane]),
            (self.acc_b.at[k, 0:o_half, :], out_o.at[ds8(k * 2 * o_half + self.core * o_half, o_half), :]),
            (self.acc_b.at[k, o_half:self.b_rows, :], out_q.at[ds8(k * 2 * q_half + self.core * q_half, q_half), :]),
        )
        far = [remote(src, dst, self.fin_send.at[k, p], self.fin_recv.at[k, p], self.peer) for p, (src, dst) in enumerate(moves)]
        near = [pltpu.make_async_copy(src, dst, self.fin_loc.at[k, p]) for p, (src, dst) in enumerate(moves)]
        return far, near

    def reduce(self, step):
        pending = []
        for k in FLOWS:
            if step == 0:
                for copy in self.core_loads(k):
                    copy.wait()
                for copy in self.core_sends(k):
                    copy.wait_recv()
                old_a, old_b = self.acc_a.at[k], self.acc_b.at[k]
            else:
                for copy in self.ici(k, step - 1):
                    copy.wait_recv()
                old_a, old_b = self.bufs_a[step - 1].at[k], self.bufs_b[step - 1].at[k]
                if step <= N_RED:
                    bit = self.gen(k, step - 1)[1]
                    old_a, old_b = self.part_a(step - 1, old_a, bit), self.part_b(step - 1, old_b, bit)
            cur_a, cur_b = self.bufs_a[step].at[k], self.bufs_b[step].at[k]
            add_rows(cur_a, old_a, cur_a.shape[0], 24)
            add_rows(cur_b, old_b, cur_b.shape[0], 16)
            if step < N_ICI:
                copies = self.ici(k, step)
            else:
                view_a, view_b = self.ag_region(k, N_RED - 1)
                view_a[...] = cur_a[...]
                view_b[...] = cur_b[...]
                copies = self.ag(k, N_RED - 1)
            for copy in pending:
                copy.start()
            pending = copies
        for copy in pending:
            copy.start()

    def grow(self, step):
        for k in FLOWS:
            for copy in self.ag(k, step + 1):
                copy.wait_recv()
            for copy in self.ag(k, step):
                copy.start()

    def finish(self):
        for k in FLOWS:
            for copy in self.ag(k, 0):
                copy.wait_recv()
            far, near = self.final(k)
            for copy in far + near:
                copy.start()

    def close(self):
        for k in FLOWS:
            for copy in self.core_sends(k):
                copy.wait_send()
            for step in range(N_ICI):
                for copy in self.ici(k, step):
                    copy.wait_send()
            for step in range(N_RED):
                for copy in self.ag(k, step):
                    copy.wait_send()
            far, near = self.final(k)
            for copy in far + near:
                copy.wait()


def comm_dims_of(grads):
    return grads[0].shape + (grads[3].shape[0], grads[4].shape[0])


def comm_scratch(dims):
    a_rows, a_lanes, q_rows, o_rows = dims
    half, lanes, b_rows = a_rows // 2, a_lanes // 2, (o_rows + q_rows) // 12
    width = o_rows
    shapes_a = [(half, lanes), (half // 2, lanes), (half // 4, lanes)] + [(half // 4, lanes // 2)] * 4
    shapes_b = [(b_rows >> min(step, N_RED), width) for step in range(N_ICI + 1)]
    dma = pltpu.SemaphoreType.DMA
    scratch = [pltpu.VMEM((6, half, lanes), F32), pltpu.VMEM((6, b_rows, width), F32)]
    scratch += [pltpu.VMEM((6,) + shape, F32) for shape in shapes_a]
    scratch += [pltpu.VMEM((6,) + shape, F32) for shape in shapes_b]
    return scratch + [dma((6, 3)), dma((6, 3)), dma((6, 3)), dma((6, N_ICI, 2)), dma((6, N_ICI, 2)), dma((6, N_RED, 2)), dma((6, N_RED, 2)), dma((6, 3)), dma((6, 3)), dma((6, 3))]


def all_reduce_kernel(dims, *refs):
    srcs, gain_ref = refs[0:5], refs[5]
    outs, out_g = refs[6:11], refs[11]
    comm = Comm(dims, srcs, outs, refs[12:38])
    gain_bufs, g_send, g_recv, g_loc = refs[38:42]

    def gain_copy(step):
        src = gain_ref if step == 0 else gain_bufs.at[step - 1]
        dev = comm.peer if step == 0 else comm.gens[step - 1][0]
        return remote(src, gain_bufs.at[step], g_send.at[step], g_recv.at[step], dev)

    comm.barrier()
    comm.open()
    gain_copy(0).start()
    for step in range(N_ICI + 1):
        comm.reduce(step)
        gain_copy(step).wait()
        gain_old = gain_ref if step == 0 else gain_bufs.at[step - 1]
        gain_bufs[step, :, :] = gain_bufs[step, :, :] + gain_old[...]
        if step < N_ICI:
            gain_copy(step + 1).start()
    gain_out = pltpu.make_async_copy(gain_bufs.at[N_ICI], out_g, g_loc)
    gain_out.start()
    comm.grow(1)
    comm.grow(0)
    comm.finish()
    gain_out.wait()
    comm.close()


def all_reduce(grads, gains):
    dims = comm_dims_of(grads)
    hbm = pl.BlockSpec(memory_space=pl.ANY)
    vmem = pl.BlockSpec(memory_space=pltpu.VMEM)
    dma = pltpu.SemaphoreType.DMA
    return pl.pallas_call(
        functools.partial(all_reduce_kernel, dims),
        in_specs=[hbm] * 5 + [vmem],
        out_specs=[hbm] * 6,
        out_shape=[jax.ShapeDtypeStruct(grad.shape, F32) for grad in grads] + [jax.ShapeDtypeStruct(gains.shape, F32)],
        scratch_shapes=comm_scratch(dims) + [pltpu.VMEM((N_ICI + 1,) + gains.shape, F32), dma((N_ICI + 1,)), dma((N_ICI + 1,)), dma],
        compiler_params=pltpu.CompilerParams(vmem_limit_bytes=40 * 1024 * 1024, collective_id=1, has_side_effects=True),
        name="all_reduce",
    )(*grads, gains)


def whole(shape):
    return pl.BlockSpec(shape, lambda *_: (0,) * len(shape))


def whole_once(shape):
    return pl.BlockSpec(shape, lambda *_: (0,) * len(shape), pipeline_mode=pl.Buffered(1))


def qkv_step(x_ref, gain_ref, w_ref, qkv):
    gain = gain_ref[...]

    @pl.loop(0, x_ref.shape[1] // BLK)
    def _(j):
        cols = ds_of(j * BLK, BLK, BLK)
        x_f = x_ref[:, cols].astype(F32)
        inv = lax.rsqrt(jnp.mean(x_f * x_f, axis=0, keepdims=True) + NORM_EPS)
        qkv[:, cols] = dot_nn(w_ref[...], (x_f * inv * gain).astype(BF16)).astype(BF16)


def attn_fwd_step(att_scale, first, q_ref, k_ref, v_ref, cos_ref, sin_ref, a_ref, qr_ref, kr_ref, st_ref, k_scr):
    n_blk = q_ref.shape[1] // BLK
    cos_t = cos_ref[...]
    sin_t = sin_ref[...]

    @pl.when(first)
    def _():
        k_f = k_ref[...].astype(F32)
        k_rot = (k_f * cos_t + pair_swap(k_f) * sin_t).astype(BF16)
        kr_ref[...] = k_rot
        k_scr[...] = k_rot.astype(F32).T.astype(BF16)

    coef = att_scale * LOG2E
    mask = diag_mask()
    q_f = q_ref[...].astype(F32)
    qr_ref[...] = (q_f * cos_t + pair_swap(q_f) * sin_t).astype(BF16)
    for j in range(n_blk):
        cols = slice(j * BLK, (j + 1) * BLK)
        q_j = qr_ref[:, cols]
        s_blocks = []
        for i in range(j + 1):
            s_i = dot_nn(k_scr[i * BLK:(i + 1) * BLK, :], q_j)
            if i == j:
                s_i = jnp.where(mask, s_i, -1e30)
            s_blocks.append(s_i)
        top = functools.reduce(jnp.maximum, [jnp.max(s_i, axis=0, keepdims=True) for s_i in s_blocks])
        e_blocks = [jnp.exp2((s_i - top) * coef) for s_i in s_blocks]
        total = functools.reduce(jnp.add, [jnp.sum(e_i, axis=0, keepdims=True) for e_i in e_blocks])
        inv = 1.0 / total
        acc = None
        for i in range(j + 1):
            p_i = (e_blocks[i] * inv).astype(BF16)
            part = dot_nn(v_ref[:, i * BLK:(i + 1) * BLK], p_i)
            acc = part if acc is None else acc + part
        a_ref[:, cols] = acc.astype(BF16)
        st_ref[0:1, cols] = top
        st_ref[1:2, cols] = inv


def attn_bwd_step(att_scale, first, last, qr_ref, kr_ref, v_ref, do_ref, st_ref, cos_ref, sin_ref, dq_ref, dk_ref, dv_ref, k_scr, v_scr, dk_acc, dv_acc):
    n_blk = qr_ref.shape[1] // BLK

    @pl.when(first)
    def _():
        k_scr[...] = kr_ref[...].astype(F32).T.astype(BF16)
        v_scr[...] = v_ref[...].astype(F32).T.astype(BF16)
        dk_acc[...] = jnp.zeros_like(dk_acc)
        dv_acc[...] = jnp.zeros_like(dv_acc)

    coef = att_scale * LOG2E
    mask = diag_mask()
    for j in range(n_blk):
        cols = slice(j * BLK, (j + 1) * BLK)
        q_j = qr_ref[:, cols]
        do_j = do_ref[:, cols]
        top = st_ref[0:1, cols]
        inv = st_ref[1:2, cols]
        p_blocks = []
        dp_blocks = []
        row_dot = None
        for i in range(j + 1):
            keys = slice(i * BLK, (i + 1) * BLK)
            s_i = dot_nn(k_scr[keys, :], q_j)
            if i == j:
                s_i = jnp.where(mask, s_i, -1e30)
            p_i = jnp.exp2((s_i - top) * coef) * inv
            dp_i = dot_nn(v_scr[keys, :], do_j).astype(BF16).astype(F32)
            part = jnp.sum(p_i * dp_i, axis=0, keepdims=True)
            row_dot = part if row_dot is None else row_dot + part
            dv_acc[:, keys] += dot_nt(do_j, p_i.astype(BF16))
            p_blocks.append(p_i)
            dp_blocks.append(dp_i)
        dq_j = None
        for i in range(j + 1):
            keys = slice(i * BLK, (i + 1) * BLK)
            ds_i = (p_blocks[i] * (dp_blocks[i] - row_dot) * att_scale).astype(BF16)
            part = dot_nn(kr_ref[:, keys], ds_i)
            dq_j = part if dq_j is None else dq_j + part
            dk_acc[:, keys] += dot_nt(q_j, ds_i)
        dq_j = dq_j.astype(BF16).astype(F32)
        dq_ref[:, cols] = (dq_j * cos_ref[:, cols] - pair_swap(dq_j) * sin_ref[:, cols]).astype(BF16)

    @pl.when(last)
    def _():
        d_k = dk_acc[...].astype(BF16).astype(F32)
        dk_ref[...] = (d_k * cos_ref[...] - pair_swap(d_k) * sin_ref[...]).astype(BF16)
        dv_ref[...] = dv_acc[...].astype(BF16)


def input_step(scale, x_ref, dmid_ref, gain_ref, w_ref, dqkv, dx_ref, gw_ref, gg_ref, w_t, gacc):
    gacc[...] = jnp.zeros_like(gacc)
    gw_ref[...] = jnp.zeros_like(gw_ref)
    gain = gain_ref[...]
    w_t[...] = w_ref[...].T

    @pl.loop(0, x_ref.shape[1] // BLK)
    def _(j):
        cols = ds_of(j * BLK, BLK, BLK)
        x_f = x_ref[:, cols].astype(F32)
        inv = lax.rsqrt(jnp.mean(x_f * x_f, axis=0, keepdims=True) + NORM_EPS)
        normed = (x_f * inv * gain).astype(BF16)
        gw_ref[...] += dot_nt(dqkv[:, cols], normed)
        d_normed = dot_nn(w_t[...], dqkv[:, cols]).astype(BF16).astype(F32)
        d_resid, d_gain = norm_back_cols(x_f, inv, gain, d_normed)
        gacc[...] += fold_lanes(d_gain)
        dx_ref[:, cols] = (dmid_ref[:, cols].astype(F32) + d_resid).astype(BF16)

    gw_ref[...] = gw_ref[...] * scale
    gg_ref[...] = jnp.sum(gacc[...], axis=1, keepdims=True) * scale


def ffn_step(scale, first, last, x_ref, a_ref, dout_ref, wo_ref, gain_ref, wg_ref, wu_ref, wd_ref, gwo_ref, gg_ref, gwg_ref, gwu_ref, gwd_ref, m_scr, n_scr, inv_scr, acc, hid, dg, du, wg_t, wu_t, wd_t, wo_t, gacc):
    n_blk = x_ref.shape[1] // BLK
    gain = gain_ref[...]

    @pl.when(first)
    def _():
        wo_t[...] = wo_ref[...].T

        @pl.loop(0, n_blk)
        def _(j):
            cols = ds_of(j * BLK, BLK, BLK)
            m_b = (x_ref[:, cols].astype(F32) + dot_nn(wo_t[...], a_ref[:, cols])).astype(BF16)
            m_scr[:, cols] = m_b
            m_f = m_b.astype(F32)
            inv = lax.rsqrt(jnp.mean(m_f * m_f, axis=0, keepdims=True) + NORM_EPS)
            inv_scr[0:1, cols] = inv
            n_scr[:, cols] = (m_f * inv * gain).astype(BF16)
        acc[...] = jnp.zeros_like(acc)
        gacc[...] = jnp.zeros_like(gacc)

    wg_t[...] = wg_ref[...].T
    wu_t[...] = wu_ref[...].T
    wd_t[...] = wd_ref[...].T
    for j in range(n_blk):
        cols = slice(j * BLK, (j + 1) * BLK)
        gate_f = dot_nn(wg_t[...], n_scr[:, cols]).astype(BF16).astype(F32)
        up_f = dot_nn(wu_t[...], n_scr[:, cols]).astype(BF16).astype(F32)
        d_hidden = dot_nn(wd_t[...], dout_ref[:, cols]).astype(BF16).astype(F32)
        gate_sig = jax.nn.sigmoid(gate_f)
        silu_act = gate_f * gate_sig
        hid[:, cols] = (silu_act * up_f).astype(BF16)
        dg[:, cols] = (d_hidden * up_f * gate_sig * (1.0 + gate_f * (1.0 - gate_sig))).astype(BF16)
        du[:, cols] = (d_hidden * silu_act).astype(BF16)
        acc[:, cols] += dot_nn(wg_ref[...], dg[:, cols]) + dot_nn(wu_ref[...], du[:, cols])
    gwg_ref[...] = dot_nt(n_scr[...], dg[...]) * scale
    gwu_ref[...] = dot_nt(n_scr[...], du[...]) * scale
    gwd_ref[...] = dot_nt(dout_ref[...], hid[...]) * scale

    @pl.when(last)
    def _():
        gwo_ref[...] = jnp.zeros_like(gwo_ref)

        @pl.loop(0, n_blk)
        def _(j):
            cols = ds_of(j * BLK, BLK, BLK)
            d_normed = acc[:, cols].astype(BF16).astype(F32)
            d_resid, d_gain = norm_back_cols(m_scr[:, cols].astype(F32), inv_scr[0:1, cols], gain, d_normed)
            gacc[...] += fold_lanes(d_gain)
            d_mid = (dout_ref[:, cols].astype(F32) + d_resid).astype(BF16)
            gwo_ref[...] += dot_nt(a_ref[:, cols], d_mid)
            m_scr[:, cols] = d_mid
            a_ref[:, cols] = dot_nn(wo_ref[...], d_mid).astype(BF16)

        gwo_ref[...] = gwo_ref[...] * scale
        gg_ref[...] = jnp.sum(gacc[...], axis=1, keepdims=True) * scale


COMM_AT = ((0, "open"), (5, 0), (11, 1), (13, 2), (14, 3), (15, 4), (17, 5), (19, 6), (21, "grow1"), (23, "grow0"))


def layer_kernel(scale, dims, comm_dims, *refs):
    kv_heads, n_group, head_dim = dims
    n_src = 5 if comm_dims else 0
    refs = list(refs)
    x_ref, dout_ref, wqkv_ref, wo_ref, ga_ref, gf_ref, cos_ref, sin_ref, wg_ref, wu_ref, wd_ref = refs[:11]
    srcs = refs[11:11 + n_src]
    pos = 11 + n_src
    dx_ref, gwqkv_ref, gwo_ref, gga_ref, ggf_ref, gwg_ref, gwu_ref, gwd_ref = refs[pos:pos + 8]
    outs = refs[pos + 8:pos + 8 + n_src]
    pos = pos + 8 + n_src
    qkv, a_scr, qr, kr, st, k_scr, v_scr, dk_acc, dv_acc, m_scr, n_scr, inv_scr, acc, hid, dg, du, wg_t, wu_t, wd_t, wo_t, wqkv_t, gacc = refs[pos:pos + 22]
    comm_refs = refs[pos + 22:]
    step = pl.program_id(0)
    heads = kv_heads * n_group
    n_ffn = pl.num_programs(0) - 2 * heads
    att_scale = head_dim ** -0.5
    per = (n_group + 2) * head_dim

    if comm_dims:
        comm = Comm(comm_dims, srcs, outs, comm_refs)
        for at, stage in COMM_AT:
            @pl.when(step == at)
            def _(stage=stage):
                if stage == "open":
                    comm.barrier()
                    comm.open()
                elif stage == "grow1":
                    comm.grow(1)
                elif stage == "grow0":
                    comm.grow(0)
                else:
                    comm.reduce(stage)

    @pl.when(step == 0)
    def _():
        qkv_step(x_ref, ga_ref, wqkv_ref, qkv)

    def head_views(idx):
        g, h = idx // n_group, lax.rem(idx, n_group)
        base = g * per
        rows_q = ds_of(base + h * head_dim, head_dim, head_dim)
        rows_k = ds_of(base + n_group * head_dim, head_dim, head_dim)
        rows_v = ds_of(base + (n_group + 1) * head_dim, head_dim, head_dim)
        return h, qkv.at[rows_q, :], qkv.at[rows_k, :], qkv.at[rows_v, :], a_scr.at[ds_of(idx * head_dim, head_dim, head_dim), :], qr.at[ds_of(idx * head_dim, head_dim, head_dim), :], kr.at[ds_of(g * head_dim, head_dim, head_dim), :], st.at[idx]

    @pl.when(step < heads)
    def _():
        h, q_v, k_v, v_v, a_v, qr_v, kr_v, st_v = head_views(step)
        attn_fwd_step(att_scale, h == 0, q_v, k_v, v_v, cos_ref, sin_ref, a_v, qr_v, kr_v, st_v, k_scr)

    @pl.when((step >= heads) & (step < heads + n_ffn))
    def _():
        ffn_step(scale, step == heads, step == heads + n_ffn - 1, x_ref, a_scr, dout_ref, wo_ref, gf_ref, wg_ref, wu_ref, wd_ref, gwo_ref, ggf_ref, gwg_ref, gwu_ref, gwd_ref, m_scr, n_scr, inv_scr, acc, hid, dg, du, wg_t, wu_t, wd_t, wo_t, gacc)

    @pl.when(step >= heads + n_ffn)
    def _():
        h, q_v, k_v, v_v, a_v, qr_v, kr_v, st_v = head_views(step - heads - n_ffn)
        attn_bwd_step(att_scale, h == 0, h == n_group - 1, qr_v, kr_v, v_v, a_v, st_v, cos_ref, sin_ref, q_v, k_v, v_v, k_scr, v_scr, dk_acc, dv_acc)

    @pl.when(step == pl.num_programs(0) - 1)
    def _():
        input_step(scale, x_ref, m_scr, ga_ref, wqkv_ref, qkv, dx_ref, gwqkv_ref, gga_ref, wqkv_t, gacc)
        if comm_dims:
            comm.finish()
            comm.close()


def layer_call(x_t, d_out_t, weights, cos_t, sin_t, scale, dims, other=None):
    g_attn, wqkv_t, w_o, g_ffn, w_gate, w_up, wd_t = weights
    kv_heads, n_group, head_dim = dims
    model_dim, seq_len = x_t.shape
    ff_dim = w_gate.shape[1]
    heads = kv_heads * n_group
    n_ffn = ff_dim // BLK
    w_spec = pl.BlockSpec((model_dim, BLK), lambda t: (0, jnp.minimum(jnp.maximum(t - heads, 0), n_ffn - 1)))
    hbm = pl.BlockSpec(memory_space=pl.ANY)
    col = (model_dim, 1)
    in_specs = [whole_once(x_t.shape), whole_once(x_t.shape), whole_once(wqkv_t.shape), whole_once(w_o.shape), whole_once(col), whole_once(col), whole_once(cos_t.shape), whole_once(cos_t.shape), w_spec, w_spec, w_spec]
    args = [x_t, d_out_t, wqkv_t, w_o, g_attn, g_ffn, cos_t, sin_t, w_gate, w_up, wd_t]
    out_specs = [whole_once(x_t.shape), whole_once(wqkv_t.shape), whole_once(w_o.shape), whole_once(col), whole_once(col), w_spec, w_spec, w_spec]
    shape = jax.ShapeDtypeStruct
    out_shape = [shape(x_t.shape, BF16), shape(wqkv_t.shape, F32), shape(w_o.shape, F32), shape(col, F32), shape(col, F32)] + [shape(w_gate.shape, F32)] * 3
    vm = pltpu.VMEM
    tok = (seq_len, head_dim)
    scratch = [vm(wqkv_t.shape[:1] + (seq_len,), BF16), vm((heads * head_dim, seq_len), BF16), vm((heads * head_dim, seq_len), BF16), vm((kv_heads * head_dim, seq_len), BF16), vm((heads, 8, seq_len), F32)]
    scratch += [vm(tok, BF16), vm(tok, BF16), vm(tok[::-1], F32), vm(tok[::-1], F32), vm(x_t.shape, BF16), vm(x_t.shape, BF16), vm((8, seq_len), F32), vm(x_t.shape, F32)]
    scratch += [vm((BLK, seq_len), BF16)] * 3 + [vm((BLK, model_dim), BF16)] * 3 + [vm(w_o.shape[::-1], BF16), vm(wqkv_t.shape[::-1], BF16), vm((model_dim, 128), F32)]
    comm_dims = None
    params = {}
    if other is not None:
        comm_dims = comm_dims_of(other)
        args += list(other)
        in_specs += [hbm] * 5
        out_specs += [hbm] * 5
        out_shape += [shape(grad.shape, F32) for grad in other]
        scratch += comm_scratch(comm_dims)
        params = dict(collective_id=0, has_side_effects=True)
    flops = 24 * x_t.size * ff_dim
    return pl.pallas_call(
        functools.partial(layer_kernel, scale, dims, comm_dims),
        grid=(2 * heads + n_ffn,),
        in_specs=in_specs,
        out_specs=out_specs,
        out_shape=out_shape,
        scratch_shapes=scratch,
        compiler_params=pltpu.CompilerParams(vmem_limit_bytes=67000000, **params),
        cost_estimate=pl.CostEstimate(flops=flops, bytes_accessed=20 * w_gate.size, transcendentals=0),
        name="layer" if other is None else "layer_and_sum",
    )(*args)


def solution(mesh):
    num_devices = mesh.shape["dp"]
    act_spec = P("dp", None, None)
    rep_spec = P()

    def local_step(x_layer0, x_layer1, d_out, g_attn, w_q, w_k, w_v, w_o, g_ffn, w_gate, w_up, w_down):
        _, seq_len, model_dim = x_layer0.shape
        n_heads, head_dim = w_q.shape[2], w_q.shape[3]
        kv_heads = w_k.shape[2]
        n_group = n_heads // kv_heads
        per = (n_group + 2) * head_dim
        cos_np, sin_np = rope_tables_np(seq_len, head_dim)
        cos_t, sin_t = jnp.asarray(cos_np), jnp.asarray(sin_np)
        scale = 1.0 / num_devices

        def layer_weights(layer):
            def heads_out(w):
                return jnp.transpose(w[layer], (1, 2, 0)).reshape(kv_heads, -1, model_dim)
            wqkv_t = jnp.concatenate([heads_out(w_q), heads_out(w_k), heads_out(w_v)], axis=1).reshape(-1, model_dim)
            return (g_attn[layer].astype(F32)[:, None], wqkv_t, w_o[layer].reshape(-1, model_dim), g_ffn[layer].astype(F32)[:, None], w_gate[layer], w_up[layer], jnp.transpose(w_down[layer], (1, 0)))

        x0_t = jnp.transpose(x_layer0[0], (1, 0))
        x1_t = jnp.transpose(x_layer1[0], (1, 0))
        d_top = jnp.transpose(d_out[0], (1, 0))
        w_low, w_top = layer_weights(0), layer_weights(1)
        dims = (kv_heads, n_group, head_dim)
        d_mid, gq1, go1, ga1, gf1, gg1, gu1, gd1 = layer_call(x1_t, d_top, w_top, cos_t, sin_t, scale, dims)
        low = layer_call(x0_t, d_mid, w_low, cos_t, sin_t, scale, dims, (gg1, gu1, gd1, gq1, go1))
        d_x0, gq0, go0, ga0, gf0, gg0, gu0, gd0 = low[:8]
        zero_col = jnp.zeros((model_dim, 4), F32)
        gains = jnp.concatenate([ga0, gf0, ga1, gf1, zero_col], axis=1).T
        sums = all_reduce((gg0, gu0, gd0, gq0, go0), gains)
        sum_g = sums[5]
        sum_gate, sum_up, sum_wd, sum_q, sum_o = [jnp.stack([first, second]) for first, second in zip(sums[:5], low[8:])]
        by_group = sum_q.reshape(2, kv_heads, per, model_dim)

        def heads_in(g):
            return jnp.transpose(g.reshape(2, -1, head_dim, model_dim), (0, 3, 1, 2))

        q_end, k_end = n_group * head_dim, (n_group + 1) * head_dim
        d_x = jnp.transpose(d_x0, (1, 0))[None]
        return (d_x, sum_g[0:4:2], heads_in(by_group[:, :, :q_end]), heads_in(by_group[:, :, q_end:k_end]), heads_in(by_group[:, :, k_end:]), sum_o.reshape(2, n_heads, head_dim, model_dim), sum_g[1:4:2], sum_gate, sum_up, jnp.transpose(sum_wd, (0, 2, 1)))

    return jax.shard_map(local_step, mesh=mesh, in_specs=(act_spec, act_spec, act_spec) + (rep_spec,) * 9, out_specs=(act_spec,) + (rep_spec,) * 9, check_vma=False)
```

```python
import functools

import jax
import jax.numpy as jnp
import numpy as np
from jax import lax
from jax.experimental import pallas as pl
from jax.experimental.pallas import tpu as pltpu
from jax.sharding import PartitionSpec as P

NORM_EPS = 1e-6
ROPE_THETA = 10000.0
BLK = 256
VMEM_ALL = 67000000
VMEM_PART = 67000000
LOG2E = 1.4426950408889634
F32 = jnp.float32
BF16 = jnp.bfloat16


def rope_tables_np(seq_len, head_dim):
    positions = np.arange(seq_len, dtype=np.float32)
    inv_freq = np.float32(ROPE_THETA) ** (-np.arange(0, head_dim, 2, dtype=np.float32) / np.float32(head_dim))
    angles = (positions[None, :] * inv_freq.astype(np.float32)[:, None]).astype(np.float32)
    cos_t = np.repeat(np.cos(angles), 2, axis=0).astype(np.float32)
    sin_t = np.repeat(np.sin(angles), 2, axis=0).astype(np.float32)
    sin_t[0::2] *= -1.0
    return cos_t, sin_t


def pair_swap(values):
    rows = values.shape[0]
    even = lax.broadcasted_iota(jnp.int32, values.shape, 0) % 2 == 0
    return jnp.where(even, pltpu.roll(values, rows - 1, 0), pltpu.roll(values, 1, 0))


def dot_nn(lhs, rhs):
    return lax.dot_general(lhs, rhs, (((1,), (0,)), ((), ())), preferred_element_type=F32)


def dot_nt(lhs, rhs):
    return lax.dot_general(lhs, rhs, (((1,), (1,)), ((), ())), preferred_element_type=F32)


def diag_mask():
    keys = lax.broadcasted_iota(jnp.int32, (BLK, BLK), 0)
    queries = lax.broadcasted_iota(jnp.int32, (BLK, BLK), 1)
    return queries >= keys


def ds_of(start, size, align):
    return pl.ds(pl.multiple_of(start, align), size)


def norm_back_cols(x_f, inv, gain, d_normed):
    scaled = d_normed * gain
    d_resid = inv * scaled - x_f * (inv * inv * inv) * jnp.mean(scaled * x_f, axis=0, keepdims=True)
    return d_resid, d_normed * x_f * inv


def fold_lanes(values):
    return functools.reduce(jnp.add, [values[:, i:i + 128] for i in range(0, values.shape[1], 128)])


MESH = pl.DeviceIdType.MESH
N_RED = 3
N_ICI = 6
SUM_SUB = 2
LAYER_SUB = 2
ADD_ROWS = 72
LANE = 128


def ds8(start, size):
    return ds_of(start, size, 8)


def remote(src, dst, send, recv, dev):
    return pltpu.make_async_remote_copy(src_ref=src, dst_ref=dst, send_sem=send, recv_sem=recv, device_id=(dev,), device_id_type=MESH)


def add_rows(dst, src):
    @pl.loop(0, dst.shape[0] // ADD_ROWS)
    def _(i):
        part = ds8(i * ADD_ROWS, ADD_ROWS)
        dst[part, :] = dst[part, :] + src[part, :]


class Comm:
    def __init__(self, n_sub, srcs, outs, refs):
        rows, width = srcs[0].shape
        self.n_sub, self.n_flow = n_sub, N_ICI * n_sub
        self.srcs, self.outs = srcs, outs
        self.acc, self.bufs = refs[0], refs[1:8]
        (self.core_send, self.core_recv, self.load_sem, self.ici_send, self.ici_recv, self.ag_send, self.ag_recv, self.fin_send, self.fin_recv, self.fin_loc) = refs[8:18]
        self.half, self.width, self.lanes = rows // 2, width, len(srcs) * width // self.n_flow
        me = lax.axis_index("dp")
        self.core = lax.rem(me, 2)
        self.peer = me + 1 - 2 * self.core
        self.gens = []
        for kind in range(2):
            for stride in (2, 8, 32):
                v = lax.rem(me // stride, 4)
                if kind == 0:
                    partner, bit = v + 1 - 2 * lax.rem(v, 2), lax.rem(v + v // 2, 2)
                else:
                    partner, bit = 3 - v, v // 2
                self.gens.append((me + (partner - v) * stride, bit))

    def barrier(self):
        barrier = pltpu.get_barrier_semaphore()
        for dev in [self.peer] + [g[0] for g in self.gens]:
            pl.semaphore_signal(barrier, inc=1, device_id=(dev,), device_id_type=MESH)
        pl.semaphore_wait(barrier, 1 + N_ICI)

    def flows(self, sub):
        return range(N_ICI * sub, N_ICI * (sub + 1))

    def gen(self, f, step):
        return self.gens[(f + step) % N_ICI]

    def bands(self, f):
        low, high = f * self.lanes, (f + 1) * self.lanes
        found = []
        while low < high:
            mat = low // self.width
            end = min(high, (mat + 1) * self.width)
            found.append((mat, slice(low - mat * self.width, end - mat * self.width), slice(low - f * self.lanes, end - f * self.lanes)))
            low = end
        return found

    def core_sends(self, f):
        rows = ds8((1 - self.core) * self.half, self.half)
        return [remote(self.srcs[mat].at[rows, cols], self.bufs[0].at[f, :, own], self.core_send.at[f, p], self.core_recv.at[f, p], self.peer) for p, (mat, cols, own) in enumerate(self.bands(f))]

    def core_loads(self, f):
        rows = ds8(self.core * self.half, self.half)
        return [pltpu.make_async_copy(self.srcs[mat].at[rows, cols], self.acc.at[f, :, own], self.load_sem.at[f, p]) for p, (mat, cols, own) in enumerate(self.bands(f))]

    def final(self, f):
        rows = ds8(self.core * self.half, self.half)
        moves = [(self.acc.at[f, :, own], self.outs[mat].at[rows, cols]) for mat, cols, own in self.bands(f)]
        far = [remote(src, dst, self.fin_send.at[f, p], self.fin_recv.at[f, p], self.peer) for p, (src, dst) in enumerate(moves)]
        near = [pltpu.make_async_copy(src, dst, self.fin_loc.at[f, p]) for p, (src, dst) in enumerate(moves)]
        return far, near

    def open(self, sub):
        for f in self.flows(sub):
            for copy in self.core_sends(f) + self.core_loads(f):
                copy.start()

    def part(self, step, buf, bit):
        if step < N_RED - 1:
            size = self.half >> (step + 1)
            return buf.at[ds8(bit * size, size), :]
        return buf.at[:, ds_of(bit * (self.lanes // 2), self.lanes // 2, LANE)]

    def ici(self, f, step):
        dev, bit = self.gen(f, step)
        src = self.bufs[step].at[f]
        if step < N_RED:
            src = self.part(step, src, 1 - bit)
        return remote(src, self.bufs[step + 1].at[f], self.ici_send.at[f, step], self.ici_recv.at[f, step], dev)

    def region(self, f, step):
        bits = [self.gen(f, s)[1] for s in range(N_RED)]
        top = min(step, N_RED - 2)
        rows = ds8(sum([bits[s] * (self.half >> (s + 1)) for s in range(top + 1)]), self.half >> (top + 1))
        if step < N_RED - 1:
            return self.acc.at[f, rows, :]
        return self.acc.at[f, rows, ds_of(bits[step] * (self.lanes // 2), self.lanes // 2, LANE)]

    def ag(self, f, step):
        view = self.region(f, step)
        return remote(view, view, self.ag_send.at[f, step], self.ag_recv.at[f, step], self.gen(f, step)[0])

    def reduce(self, step, sub):
        pending = None
        for f in self.flows(sub):
            if step == 0:
                for copy in self.core_loads(f):
                    copy.wait()
                for copy in self.core_sends(f):
                    copy.wait_recv()
                old = self.acc.at[f]
            else:
                self.ici(f, step - 1).wait_recv()
                old = self.bufs[step - 1].at[f]
                if step <= N_RED:
                    old = self.part(step - 1, old, self.gen(f, step - 1)[1])
            cur = self.bufs[step].at[f]
            add_rows(cur, old)
            if step < N_ICI:
                copy = self.ici(f, step)
            else:
                view = self.region(f, N_RED - 1)
                view[...] = cur[...]
                copy = self.ag(f, N_RED - 1)
            if pending is not None:
                pending.start()
            pending = copy
        pending.start()

    def grow(self, step, sub):
        for f in self.flows(sub):
            self.ag(f, step + 1).wait_recv()
            self.ag(f, step).start()

    def finish(self, sub):
        for f in self.flows(sub):
            self.ag(f, 0).wait_recv()
            far, near = self.final(f)
            for copy in far + near:
                copy.start()

    def serve(self, stage, sub):
        if stage == 0:
            self.open(sub)
        elif stage < N_ICI + 2:
            self.reduce(stage - 1, sub)
        elif stage < N_ICI + 4:
            self.grow(N_ICI + 3 - stage, sub)
        else:
            self.finish(sub)

    def close(self):
        for f in range(self.n_flow):
            for copy in self.core_sends(f):
                copy.wait_send()
            for step in range(N_ICI):
                self.ici(f, step).wait_send()
            for step in range(N_RED):
                self.ag(f, step).wait_send()
            far, near = self.final(f)
            for copy in far + near:
                copy.wait()


def comm_scratch(n_sub, srcs):
    rows, width = srcs[0].shape
    n = N_ICI * n_sub
    half, lanes = rows // 2, len(srcs) * width // n
    shapes = [(half, lanes), (half // 2, lanes), (half // 4, lanes)] + [(half // 4, lanes // 2)] * 4
    pieces = 3 - n_sub
    dma = pltpu.SemaphoreType.DMA
    return [pltpu.VMEM((n, half, lanes), F32)] + [pltpu.VMEM((n,) + shape, F32) for shape in shapes] + [dma((n, pieces))] * 3 + [dma((n, N_ICI))] * 2 + [dma((n, N_RED))] * 2 + [dma((n, pieces))] * 3


def all_reduce_kernel(n_mat, *refs):
    srcs, gain_low, gain_top = refs[:n_mat], refs[n_mat], refs[n_mat + 1]
    refs = refs[n_mat + 2:]
    outs, out_g = refs[:n_mat], refs[n_mat]
    gain_src, gain_bufs, g_send, g_recv, g_loc = refs[-5:]
    comm = Comm(SUM_SUB, srcs, outs, refs[n_mat + 1:])

    def gain_copy(step):
        src = gain_src if step == 0 else gain_bufs.at[step - 1]
        dev = comm.peer if step == 0 else comm.gens[step - 1][0]
        return remote(src, gain_bufs.at[step], g_send.at[step], g_recv.at[step], dev)

    gain_src[...] = gain_low[...]
    gain_src[2:4, :] = gain_top[0:2, :]
    comm.barrier()
    for sub in range(SUM_SUB):
        comm.open(sub)
    gain_copy(0).start()
    for step in range(N_ICI + 1):
        for sub in range(SUM_SUB):
            comm.reduce(step, sub)
        gain_copy(step).wait()
        gain_old = gain_src if step == 0 else gain_bufs.at[step - 1]
        gain_bufs[step, :, :] = gain_bufs[step, :, :] + gain_old[...]
        if step < N_ICI:
            gain_copy(step + 1).start()
    gain_out = pltpu.make_async_copy(gain_bufs.at[N_ICI], out_g, g_loc)
    gain_out.start()
    for step in (1, 0):
        for sub in range(SUM_SUB):
            comm.grow(step, sub)
    for sub in range(SUM_SUB):
        comm.finish(sub)
    gain_out.wait()
    comm.close()


def all_reduce(grads, gain_low, gain_top):
    hbm = pl.BlockSpec(memory_space=pl.ANY)
    vmem = pl.BlockSpec(memory_space=pltpu.VMEM)
    dma = pltpu.SemaphoreType.DMA
    n_mat = len(grads)
    return pl.pallas_call(
        functools.partial(all_reduce_kernel, n_mat),
        in_specs=[hbm] * n_mat + [vmem] * 2,
        out_specs=[hbm] * (n_mat + 1),
        out_shape=[jax.ShapeDtypeStruct(grad.shape, F32) for grad in grads] + [jax.ShapeDtypeStruct(gain_low.shape, F32)],
        scratch_shapes=comm_scratch(SUM_SUB, grads) + [pltpu.VMEM(gain_low.shape, F32), pltpu.VMEM((N_ICI + 1,) + gain_low.shape, F32), dma((N_ICI + 1,)), dma((N_ICI + 1,)), dma],
        compiler_params=pltpu.CompilerParams(vmem_limit_bytes=VMEM_PART, collective_id=1, has_side_effects=True),
        name="all_reduce",
    )(*grads, gain_low, gain_top)


def assemble_kernel(n_group, *refs):
    low, top, (sum_g, dx_in), outs = refs[:4], refs[4:8], refs[8:10], refs[10:17]
    grad_ga, grad_gf, dx_out, turned = refs[17:]
    layer, i = pl.program_id(0), pl.program_id(1)
    head_dim = outs[-1].shape[0]
    base = (i // n_group) * (n_group + 2)

    def fill(mats):
        for src, dst in zip(mats[:3], outs):
            dst[...] = src[...]

        @pl.when(i == 0)
        def _():
            turned[...] = mats[-1][...].T

    @pl.when(layer == 0)
    def _():
        fill(low)
        dx_out[...] = dx_in[...]
        for row in range(2):
            grad_ga[row:row + 1, :] = sum_g[2 * row:2 * row + 1, :]
            grad_gf[row:row + 1, :] = sum_g[2 * row + 1:2 * row + 2, :]

    @pl.when(layer == 1)
    def _():
        fill(top)

    spots = (base + lax.rem(i, n_group), base + n_group, base + n_group + 1, i + pl.num_programs(1) * (n_group + 2) // n_group)
    for spot, dst in zip(spots, outs[3:]):
        dst[...] = turned[ds_of(spot * head_dim, head_dim, head_dim), :]


def assemble(low, top, sum_g, d_x, n_group, head_dim):
    model_dim, ff_dim = low[0].shape
    heads = model_dim // head_dim
    kv_heads = heads // n_group

    def maps(layer):
        def at(l, i):
            return i * (1 - l) + (heads - 1) * l if layer == 0 else i * l
        return [pl.BlockSpec((head_dim, ff_dim), lambda l, i: (at(l, i), 0))] * 3 + [pl.BlockSpec(low[3].shape, lambda l, i: (0, 0), pipeline_mode=pl.Buffered(1))]

    out_big = pl.BlockSpec((None, head_dim, ff_dim), lambda l, i: (l, i, 0))
    out_small = pl.BlockSpec((None, head_dim, model_dim), lambda l, i: (l, i, 0))
    out_kv = pl.BlockSpec((None, head_dim, model_dim), lambda l, i: (l, i // n_group, 0))
    shape = jax.ShapeDtypeStruct
    gain_shape = shape((2, model_dim), F32)
    dx_spec = pl.BlockSpec((head_dim, d_x.shape[1]), lambda l, i: (i * (1 - l) + (heads - 1) * l, 0))
    big_shape, q_shape, kv_shape = shape((2, model_dim, ff_dim), F32), shape((2, model_dim, model_dim), F32), shape((2, kv_heads * head_dim, model_dim), F32)
    return pl.pallas_call(
        functools.partial(assemble_kernel, n_group),
        grid=(2, heads),
        in_specs=maps(0) + maps(1) + [whole_once(sum_g.shape), dx_spec],
        out_specs=[out_big] * 3 + [out_small, out_kv, out_kv, out_small, whole_once(gain_shape.shape), whole_once(gain_shape.shape), dx_spec],
        out_shape=[big_shape] * 3 + [q_shape, kv_shape, kv_shape, q_shape, gain_shape, gain_shape, shape(d_x.shape, d_x.dtype)],
        scratch_shapes=[pltpu.VMEM(low[3].shape[::-1], F32)],
        compiler_params=pltpu.CompilerParams(vmem_limit_bytes=VMEM_PART),
        name="assemble",
    )(*low, *top, sum_g, d_x)


def whole_once(shape):
    return pl.BlockSpec(shape, lambda *_: (0,) * len(shape), pipeline_mode=pl.Buffered(1))


def qkv_step(x_ref, gain_ref, w_ref, qkv):
    gain = gain_ref[...]

    @pl.loop(0, x_ref.shape[1] // BLK)
    def _(j):
        cols = ds_of(j * BLK, BLK, BLK)
        x_f = x_ref[:, cols].astype(F32)
        inv = lax.rsqrt(jnp.mean(x_f * x_f, axis=0, keepdims=True) + NORM_EPS)
        qkv[:, cols] = dot_nn(w_ref[...], (x_f * inv * gain).astype(BF16)).astype(BF16)


def attn_fwd_step(att_scale, first, q_ref, k_ref, v_ref, cos_ref, sin_ref, a_ref, qr_ref, kr_ref, st_ref, k_scr):
    n_blk = q_ref.shape[1] // BLK
    cos_t = cos_ref[...]
    sin_t = sin_ref[...]

    @pl.when(first)
    def _():
        k_f = k_ref[...].astype(F32)
        k_rot = (k_f * cos_t + pair_swap(k_f) * sin_t).astype(BF16)
        kr_ref[...] = k_rot
        k_scr[...] = k_rot.astype(F32).T.astype(BF16)

    coef = att_scale * LOG2E
    mask = diag_mask()
    q_f = q_ref[...].astype(F32)
    qr_ref[...] = (q_f * cos_t + pair_swap(q_f) * sin_t).astype(BF16)
    for j in range(n_blk):
        cols = slice(j * BLK, (j + 1) * BLK)
        q_j = qr_ref[:, cols]
        s_blocks = []
        for i in range(j + 1):
            s_i = dot_nn(k_scr[i * BLK:(i + 1) * BLK, :], q_j)
            if i == j:
                s_i = jnp.where(mask, s_i, -1e30)
            s_blocks.append(s_i)
        top = functools.reduce(jnp.maximum, [jnp.max(s_i, axis=0, keepdims=True) for s_i in s_blocks])
        e_blocks = [jnp.exp2((s_i - top) * coef) for s_i in s_blocks]
        total = functools.reduce(jnp.add, [jnp.sum(e_i, axis=0, keepdims=True) for e_i in e_blocks])
        inv = 1.0 / total
        acc = None
        for i in range(j + 1):
            p_i = (e_blocks[i] * inv).astype(BF16)
            part = dot_nn(v_ref[:, i * BLK:(i + 1) * BLK], p_i)
            acc = part if acc is None else acc + part
        a_ref[:, cols] = acc.astype(BF16)
        st_ref[0:1, cols] = top
        st_ref[1:2, cols] = inv


def clear(*targets):
    for ref in targets:
        ref[...] = jnp.zeros_like(ref)


def attn_bwd_step(att_scale, first, last, qr_ref, kr_ref, v_ref, do_ref, st_ref, cos_ref, sin_ref, dq_ref, dk_ref, dv_ref, k_scr, v_scr, dk_acc, dv_acc):
    n_blk = qr_ref.shape[1] // BLK

    @pl.when(first)
    def _():
        k_scr[...] = kr_ref[...].astype(F32).T.astype(BF16)
        v_scr[...] = v_ref[...].astype(F32).T.astype(BF16)
        clear(dk_acc)
        clear(dv_acc)

    coef = att_scale * LOG2E
    mask = diag_mask()
    for j in range(n_blk):
        cols = slice(j * BLK, (j + 1) * BLK)
        q_j = qr_ref[:, cols]
        do_j = do_ref[:, cols]
        top = st_ref[0:1, cols]
        inv = st_ref[1:2, cols]
        p_blocks = []
        dp_blocks = []
        row_dot = None
        for i in range(j + 1):
            keys = slice(i * BLK, (i + 1) * BLK)
            s_i = dot_nn(k_scr[keys, :], q_j)
            if i == j:
                s_i = jnp.where(mask, s_i, -1e30)
            p_i = jnp.exp2((s_i - top) * coef) * inv
            dp_i = dot_nn(v_scr[keys, :], do_j).astype(BF16).astype(F32)
            part = jnp.sum(p_i * dp_i, axis=0, keepdims=True)
            row_dot = part if row_dot is None else row_dot + part
            dv_acc[:, keys] += dot_nt(do_j, p_i.astype(BF16))
            p_blocks.append(p_i)
            dp_blocks.append(dp_i)
        dq_j = None
        for i in range(j + 1):
            keys = slice(i * BLK, (i + 1) * BLK)
            ds_i = (p_blocks[i] * (dp_blocks[i] - row_dot) * att_scale).astype(BF16)
            part = dot_nn(kr_ref[:, keys], ds_i)
            dq_j = part if dq_j is None else dq_j + part
            dk_acc[:, keys] += dot_nt(q_j, ds_i)
        dq_j = dq_j.astype(BF16).astype(F32)
        dq_ref[:, cols] = (dq_j * cos_ref[:, cols] - pair_swap(dq_j) * sin_ref[:, cols]).astype(BF16)

    @pl.when(last)
    def _():
        d_k = dk_acc[...].astype(BF16).astype(F32)
        dk_ref[...] = (d_k * cos_ref[...] - pair_swap(d_k) * sin_ref[...]).astype(BF16)
        dv_ref[...] = dv_acc[...].astype(BF16)


def input_step(scale, x_ref, dmid_ref, gain_ref, w_ref, dqkv, dx_ref, gw_ref, gg_ref, w_t, gacc):
    clear(gacc, gw_ref)
    gain = gain_ref[...]
    w_t[...] = w_ref[...].T

    @pl.loop(0, x_ref.shape[1] // BLK)
    def _(j):
        cols = ds_of(j * BLK, BLK, BLK)
        x_f = x_ref[:, cols].astype(F32)
        inv = lax.rsqrt(jnp.mean(x_f * x_f, axis=0, keepdims=True) + NORM_EPS)
        normed = (x_f * inv * gain).astype(BF16)
        gw_ref[...] += dot_nt(normed, dqkv[:, cols])
        d_normed = dot_nn(w_t[...], dqkv[:, cols]).astype(BF16).astype(F32)
        d_resid, d_gain = norm_back_cols(x_f, inv, gain, d_normed)
        gacc[...] += fold_lanes(d_gain)
        dx_ref[:, cols] = (dmid_ref[:, cols].astype(F32) + d_resid).astype(BF16)

    gw_ref[...] = gw_ref[...] * scale
    gg_ref[...] = jnp.sum(gacc[...].T, axis=0, keepdims=True) * scale


def ffn_step(scale, first, last, x_ref, a_ref, dout_ref, wo_ref, gain_ref, wg_ref, wu_ref, wd_ref, gwo_ref, gwo_acc, gg_ref, gwg_ref, gwu_ref, gwd_ref, m_scr, n_scr, inv_scr, acc, hid, dg, du, wg_t, wu_t, wd_t, wo_t, gacc):
    n_blk = x_ref.shape[1] // BLK
    gain = gain_ref[...]

    @pl.when(first)
    def _():
        wo_t[...] = wo_ref[...].T

        @pl.loop(0, n_blk)
        def _(j):
            cols = ds_of(j * BLK, BLK, BLK)
            m_b = (x_ref[:, cols].astype(F32) + dot_nn(wo_t[...], a_ref[:, cols])).astype(BF16)
            m_scr[:, cols] = m_b
            m_f = m_b.astype(F32)
            inv = lax.rsqrt(jnp.mean(m_f * m_f, axis=0, keepdims=True) + NORM_EPS)
            inv_scr[0:1, cols] = inv
            n_scr[:, cols] = (m_f * inv * gain).astype(BF16)
        clear(acc)
        clear(gacc)

    wg_t[...] = wg_ref[...].T
    wu_t[...] = wu_ref[...].T
    wd_t[...] = wd_ref[...].T
    for j in range(n_blk):
        cols = slice(j * BLK, (j + 1) * BLK)
        gate_f = dot_nn(wg_t[...], n_scr[:, cols]).astype(BF16).astype(F32)
        up_f = dot_nn(wu_t[...], n_scr[:, cols]).astype(BF16).astype(F32)
        d_hidden = dot_nn(wd_t[...], dout_ref[:, cols]).astype(BF16).astype(F32)
        gate_sig = jax.nn.sigmoid(gate_f)
        silu_act = gate_f * gate_sig
        hid[:, cols] = (silu_act * up_f).astype(BF16)
        dg[:, cols] = (d_hidden * up_f * gate_sig * (1.0 + gate_f * (1.0 - gate_sig))).astype(BF16)
        du[:, cols] = (d_hidden * silu_act).astype(BF16)
        acc[:, cols] += dot_nn(wg_ref[...], dg[:, cols]) + dot_nn(wu_ref[...], du[:, cols])
    gwg_ref[...] = dot_nt(n_scr[...], dg[...]) * scale
    gwu_ref[...] = dot_nt(n_scr[...], du[...]) * scale
    gwd_ref[...] = dot_nt(dout_ref[...], hid[...]) * scale

    @pl.when(last)
    def _():
        clear(gwo_acc)

        @pl.loop(0, n_blk)
        def _(j):
            cols = ds_of(j * BLK, BLK, BLK)
            d_normed = acc[:, cols].astype(BF16).astype(F32)
            d_resid, d_gain = norm_back_cols(m_scr[:, cols].astype(F32), inv_scr[0:1, cols], gain, d_normed)
            gacc[...] += fold_lanes(d_gain)
            d_mid = (dout_ref[:, cols].astype(F32) + d_resid).astype(BF16)
            gwo_acc[...] += dot_nt(d_mid, a_ref[:, cols])
            m_scr[:, cols] = d_mid
            a_ref[:, cols] = dot_nn(wo_ref[...], d_mid).astype(BF16)

        gwo_ref[...] = gwo_acc[...] * scale
        gg_ref[...] = jnp.sum(gacc[...].T, axis=0, keepdims=True) * scale


COMM_AT = ((0, 2, 7, 10, 11, 12, 13, 14, 15, 17, 20), (0, 5, 9, 11, 12, 13, 14, 15, 16, 19, 22))


def layer_kernel(layer, scale, dims, pl_steps, n_src, *refs):
    kv_heads, n_group, head_dim = dims
    refs = list(refs)
    x_ref, dout_ref, wq_ref, wk_ref, wv_ref, wo_ref, ga_in, gf_in, cos_ref, sin_ref, wg_ref, wu_ref, wd_ref = refs[:13]
    srcs = refs[13:13 + n_src]
    pos = 13 + n_src
    dx_ref, gb_ref, gains_ref, gwg_ref, gwu_ref, gwd_ref = refs[pos:pos + 6]
    outs = refs[pos + 6:pos + 6 + n_src]
    pos = pos + 6 + n_src
    qkv, a_scr, qr, kr, st, k_scr, v_scr, dk_acc, dv_acc, m_scr, n_scr, inv_scr, acc, hid, dg, du, wg_t, wu_t, wd_t, wo_t, wqkv_t, gacc, wqkv_ref, ga_ref, gf_ref, gwo_acc = refs[pos:pos + 26]
    comm_refs = refs[pos + 26:]
    step = pl.program_id(0)
    heads = kv_heads * n_group
    n_ffn = pl.num_programs(0) - 2 * heads
    att_scale = head_dim ** -0.5
    per = (n_group + 2) * head_dim

    if n_src:
        comm = Comm(LAYER_SUB, srcs, outs, comm_refs)
        for at in range(pl_steps):
            todo = [(stage, sub) for stage in range(len(COMM_AT[0])) for sub in range(LAYER_SUB) if COMM_AT[sub][stage] == at]
            if todo:
                @pl.when(step == at)
                def _(todo=todo, at=at):
                    if at == 0:
                        comm.barrier()
                    for stage, sub in todo:
                        comm.serve(stage, sub)

    @pl.when(step == 0)
    def _():
        q_rows = n_group * head_dim
        for g in range(kv_heads):
            wqkv_ref[g * per:g * per + q_rows, :] = wq_ref[g * q_rows:(g + 1) * q_rows, :]
            wqkv_ref[g * per + q_rows:g * per + q_rows + head_dim, :] = wk_ref[g * head_dim:(g + 1) * head_dim, :]
            wqkv_ref[g * per + q_rows + head_dim:(g + 1) * per, :] = wv_ref[g * head_dim:(g + 1) * head_dim, :]
        for src, dst in ((ga_in, ga_ref), (gf_in, gf_ref)):
            row = src[...].astype(F32)[layer:layer + 1, :]
            dst[...] = jnp.broadcast_to(row, (8, row.shape[1])).T[:, 0:1]
        clear(gains_ref)
        qkv_step(x_ref, ga_ref, wqkv_ref, qkv)

    def head_views(idx):
        g, h = idx // n_group, lax.rem(idx, n_group)
        base = g * per
        rows_q = ds_of(base + h * head_dim, head_dim, head_dim)
        rows_k = ds_of(base + n_group * head_dim, head_dim, head_dim)
        rows_v = ds_of(base + (n_group + 1) * head_dim, head_dim, head_dim)
        return h, qkv.at[rows_q, :], qkv.at[rows_k, :], qkv.at[rows_v, :], a_scr.at[ds_of(idx * head_dim, head_dim, head_dim), :], qr.at[ds_of(idx * head_dim, head_dim, head_dim), :], kr.at[ds_of(g * head_dim, head_dim, head_dim), :], st.at[idx]

    @pl.when(step < heads)
    def _():
        h, q_v, k_v, v_v, a_v, qr_v, kr_v, st_v = head_views(step)
        attn_fwd_step(att_scale, h == 0, q_v, k_v, v_v, cos_ref, sin_ref, a_v, qr_v, kr_v, st_v, k_scr)

    @pl.when((step >= heads) & (step < heads + n_ffn))
    def _():
        ffn_step(scale, step == heads, step == heads + n_ffn - 1, x_ref, a_scr, dout_ref, wo_ref, gf_ref, wg_ref, wu_ref, wd_ref, gb_ref.at[:, per * kv_heads:], gwo_acc, gains_ref.at[1:2, :], gwg_ref, gwu_ref, gwd_ref, m_scr, n_scr, inv_scr, acc, hid, dg, du, wg_t, wu_t, wd_t, wo_t, gacc)

    @pl.when(step >= heads + n_ffn)
    def _():
        h, q_v, k_v, v_v, a_v, qr_v, kr_v, st_v = head_views(step - heads - n_ffn)
        attn_bwd_step(att_scale, h == 0, h == n_group - 1, qr_v, kr_v, v_v, a_v, st_v, cos_ref, sin_ref, q_v, k_v, v_v, k_scr, v_scr, dk_acc, dv_acc)

    @pl.when(step == pl.num_programs(0) - 1)
    def _():
        input_step(scale, x_ref, m_scr, ga_ref, wqkv_ref, qkv, dx_ref, gb_ref.at[:, :per * kv_heads], gains_ref.at[0:1, :], wqkv_t, gacc)
        if n_src:
            comm.close()


def layer_call(layer, x_t, d_out_t, weights, cos_t, sin_t, scale, dims, other=None):
    g_attn, wq_t, wk_t, wv_t, w_o, g_ffn, w_gate, w_up, wd_t = weights
    kv_heads, n_group, head_dim = dims
    model_dim, seq_len = x_t.shape
    ff_dim = w_gate.shape[2]
    heads = kv_heads * n_group
    n_ffn = ff_dim // BLK
    qkv_rows = (heads + 2 * kv_heads) * head_dim
    w_spec = pl.BlockSpec((None, model_dim, BLK), lambda t: (layer, 0, jnp.minimum(jnp.maximum(t - heads, 0), n_ffn - 1)))
    g_spec = pl.BlockSpec((model_dim, BLK), lambda t: (0, jnp.minimum(jnp.maximum(t - heads, 0), n_ffn - 1)))
    hbm = pl.BlockSpec(memory_space=pl.ANY)

    def one(w):
        return pl.BlockSpec((None,) + w.shape[1:], lambda t: (layer, 0, 0), pipeline_mode=pl.Buffered(1))

    in_specs = [whole_once(x_t.shape), whole_once(x_t.shape), one(wq_t), one(wk_t), one(wv_t), one(w_o), whole_once(g_attn.shape), whole_once(g_ffn.shape), whole_once(cos_t.shape), whole_once(cos_t.shape), w_spec, w_spec, w_spec]
    args = [x_t, d_out_t, wq_t, wk_t, wv_t, w_o, g_attn, g_ffn, cos_t, sin_t, w_gate, w_up, wd_t]
    shape = jax.ShapeDtypeStruct
    qkv_w, o_w, grad_w, gain_w = (qkv_rows, model_dim), w_o.shape[1:], w_gate.shape[1:], (8, model_dim)
    out_specs = [whole_once(x_t.shape), whole_once(grad_w), whole_once(gain_w), g_spec, g_spec, g_spec]
    out_shape = [shape(x_t.shape, BF16), shape(grad_w, F32), shape(gain_w, F32)] + [shape(grad_w, F32)] * 3
    vm = pltpu.VMEM
    tok = (seq_len, head_dim)
    scratch = [vm((qkv_rows, seq_len), BF16), vm((heads * head_dim, seq_len), BF16), vm((heads * head_dim, seq_len), BF16), vm((kv_heads * head_dim, seq_len), BF16), vm((heads, 8, seq_len), F32)]
    scratch += [vm(tok, BF16), vm(tok, BF16), vm(tok[::-1], F32), vm(tok[::-1], F32), vm(x_t.shape, BF16), vm(x_t.shape, BF16), vm((8, seq_len), F32), vm(x_t.shape, F32)]
    scratch += [vm((BLK, seq_len), BF16)] * 3 + [vm((BLK, model_dim), BF16)] * 3 + [vm(o_w[::-1], BF16), vm(qkv_w[::-1], BF16), vm((model_dim, 128), F32), vm(qkv_w, BF16), vm((model_dim, 1), F32), vm((model_dim, 1), F32), vm(o_w, F32)]
    n_src = 0
    params = {}
    if other is not None:
        n_src = len(other)
        args += list(other)
        in_specs += [hbm] * n_src
        out_specs += [hbm] * n_src
        out_shape += [shape(grad.shape, F32) for grad in other]
        scratch += comm_scratch(LAYER_SUB, other)
        params = dict(collective_id=0, has_side_effects=True)
    return pl.pallas_call(
        functools.partial(layer_kernel, layer, scale, dims, 2 * heads + n_ffn, n_src),
        grid=(2 * heads + n_ffn,),
        in_specs=in_specs,
        out_specs=out_specs,
        out_shape=out_shape,
        scratch_shapes=scratch,
        compiler_params=pltpu.CompilerParams(vmem_limit_bytes=VMEM_ALL, **params),
        cost_estimate=pl.CostEstimate(flops=24 * x_t.size * ff_dim, bytes_accessed=20 * grad_w[0] * grad_w[1], transcendentals=0),
        name="layer" if other is None else "layer_and_sum",
    )(*args)


def solution(mesh):
    num_devices = mesh.shape["dp"]
    act_spec = P("dp", None, None)
    rep_spec = P()

    def local_step(x_layer0, x_layer1, d_out, g_attn, w_q, w_k, w_v, w_o, g_ffn, w_gate, w_up, w_down):
        _, seq_len, model_dim = x_layer0.shape
        n_heads, head_dim = w_q.shape[2], w_q.shape[3]
        kv_heads = w_k.shape[2]
        n_group = n_heads // kv_heads
        cos_np, sin_np = rope_tables_np(seq_len, head_dim)
        cos_t, sin_t = jnp.asarray(cos_np), jnp.asarray(sin_np)
        scale = 1.0 / num_devices

        def heads_out(w):
            return jnp.transpose(w, (0, 2, 3, 1)).reshape(2, -1, model_dim)

        weights = (g_attn, heads_out(w_q), heads_out(w_k), heads_out(w_v), w_o.reshape(2, -1, model_dim), g_ffn, w_gate, w_up, jnp.transpose(w_down, (0, 2, 1)))
        x0_t = jnp.transpose(x_layer0[0], (1, 0))
        x1_t = jnp.transpose(x_layer1[0], (1, 0))
        d_top = jnp.transpose(d_out[0], (1, 0))
        dims = (kv_heads, n_group, head_dim)
        d_mid, gb1, gains1, gg1, gu1, gd1 = layer_call(1, x1_t, d_top, weights, cos_t, sin_t, scale, dims)
        low = layer_call(0, x0_t, d_mid, weights, cos_t, sin_t, scale, dims, (gg1, gu1, gd1, gb1))
        d_x0, gb0, gains0, gg0, gu0, gd0 = low[:6]
        sums = all_reduce((gg0, gu0, gd0, gb0), gains0, gains1)
        sum_g = sums[4]
        sum_gate, sum_up, sum_wd, sum_q, sum_k, sum_v, sum_o, grad_ga, grad_gf, d_x0 = assemble(sums[:4], low[6:], sum_g, d_x0, n_group, head_dim)

        def heads_in(g):
            return jnp.transpose(g.reshape(2, -1, head_dim, model_dim), (0, 3, 1, 2))

        d_x = jnp.transpose(d_x0, (1, 0))[None]
        return (d_x, grad_ga, heads_in(sum_q), heads_in(sum_k), heads_in(sum_v), sum_o.reshape(2, n_heads, head_dim, model_dim), grad_gf, sum_gate, sum_up, jnp.transpose(sum_wd, (0, 2, 1)))

    return jax.shard_map(local_step, mesh=mesh, in_specs=(act_spec, act_spec, act_spec) + (rep_spec,) * 9, out_specs=(act_spec,) + (rep_spec,) * 9, check_vma=False)
```

```python
import functools

import jax
import jax.numpy as jnp
import numpy as np
from jax import lax
from jax.experimental import pallas as pl
from jax.experimental.pallas import tpu as pltpu
from jax.sharding import PartitionSpec as P

NORM_EPS = 1e-6
ROPE_THETA = 10000.0
BLK = 256
VMEM_ALL = 67000000
VMEM_PART = 67000000
LOG2E = 1.4426950408889634
F32 = jnp.float32
BF16 = jnp.bfloat16


def rope_tables_np(seq_len, head_dim):
    positions = np.arange(seq_len, dtype=np.float32)
    inv_freq = np.float32(ROPE_THETA) ** (-np.arange(0, head_dim, 2, dtype=np.float32) / np.float32(head_dim))
    angles = (positions[None, :] * inv_freq.astype(np.float32)[:, None]).astype(np.float32)
    cos_t = np.repeat(np.cos(angles), 2, axis=0).astype(np.float32)
    sin_t = np.repeat(np.sin(angles), 2, axis=0).astype(np.float32)
    sin_t[0::2] *= -1.0
    return cos_t, sin_t


def pair_swap(values):
    rows = values.shape[0]
    even = lax.broadcasted_iota(jnp.int32, values.shape, 0) % 2 == 0
    return jnp.where(even, pltpu.roll(values, rows - 1, 0), pltpu.roll(values, 1, 0))


def dot_nn(lhs, rhs):
    return lax.dot_general(lhs, rhs, (((1,), (0,)), ((), ())), preferred_element_type=F32)


def dot_nt(lhs, rhs):
    return lax.dot_general(lhs, rhs, (((1,), (1,)), ((), ())), preferred_element_type=F32)


def diag_mask():
    keys = lax.broadcasted_iota(jnp.int32, (BLK, BLK), 0)
    queries = lax.broadcasted_iota(jnp.int32, (BLK, BLK), 1)
    return queries >= keys


def ds_of(start, size, align):
    return pl.ds(pl.multiple_of(start, align), size)


def norm_back_cols(x_f, inv, gain, d_normed):
    scaled = d_normed * gain
    d_resid = inv * scaled - x_f * (inv * inv * inv) * jnp.mean(scaled * x_f, axis=0, keepdims=True)
    return d_resid, d_normed * x_f * inv


def fold_lanes(values):
    return functools.reduce(jnp.add, [values[:, i:i + 128] for i in range(0, values.shape[1], 128)])


MESH = pl.DeviceIdType.MESH
N_RED = 3
N_ICI = 6
SUM_SUB = 2
LAYER_SUB = 2
ADD_ROWS = 72
LANE = 128


def ds8(start, size):
    return ds_of(start, size, 8)


def remote(src, dst, send, recv, dev):
    return pltpu.make_async_remote_copy(src_ref=src, dst_ref=dst, send_sem=send, recv_sem=recv, device_id=(dev,), device_id_type=MESH)


def add_rows(dst, src):
    @pl.loop(0, dst.shape[0] // ADD_ROWS)
    def _(i):
        part = ds8(i * ADD_ROWS, ADD_ROWS)
        dst[part, :] = dst[part, :] + src[part, :]


class Comm:
    def __init__(self, n_sub, srcs, outs, refs):
        rows, width = srcs[0].shape
        self.n_sub, self.n_flow = n_sub, N_ICI * n_sub
        self.srcs, self.outs = srcs, outs
        self.acc, self.bufs = refs[0], refs[1:8]
        (self.core_send, self.core_recv, self.load_sem, self.ici_send, self.ici_recv, self.ag_send, self.ag_recv, self.fin_send, self.fin_recv, self.fin_loc) = refs[8:18]
        self.half, self.width, self.lanes = rows // 2, width, len(srcs) * width // self.n_flow
        me = lax.axis_index("dp")
        self.core = lax.rem(me, 2)
        self.peer = me + 1 - 2 * self.core
        self.gens = []
        for kind in range(2):
            for stride in (2, 8, 32):
                v = lax.rem(me // stride, 4)
                if kind == 0:
                    partner, bit = v + 1 - 2 * lax.rem(v, 2), lax.rem(v + v // 2, 2)
                else:
                    partner, bit = 3 - v, v // 2
                self.gens.append((me + (partner - v) * stride, bit))

    def barrier(self):
        barrier = pltpu.get_barrier_semaphore()
        for dev in [self.peer] + [g[0] for g in self.gens]:
            pl.semaphore_signal(barrier, inc=1, device_id=(dev,), device_id_type=MESH)
        pl.semaphore_wait(barrier, 1 + N_ICI)

    def flows(self, sub):
        return range(N_ICI * sub, N_ICI * (sub + 1))

    def gen(self, f, step):
        return self.gens[(f + step) % N_ICI]

    def bands(self, f):
        low, high = f * self.lanes, (f + 1) * self.lanes
        found = []
        while low < high:
            mat = low // self.width
            end = min(high, (mat + 1) * self.width)
            found.append((mat, slice(low - mat * self.width, end - mat * self.width), slice(low - f * self.lanes, end - f * self.lanes)))
            low = end
        return found

    def core_sends(self, f):
        rows = ds8((1 - self.core) * self.half, self.half)
        return [remote(self.srcs[mat].at[rows, cols], self.bufs[0].at[f, :, own], self.core_send.at[f, p], self.core_recv.at[f, p], self.peer) for p, (mat, cols, own) in enumerate(self.bands(f))]

    def core_loads(self, f):
        rows = ds8(self.core * self.half, self.half)
        return [pltpu.make_async_copy(self.srcs[mat].at[rows, cols], self.acc.at[f, :, own], self.load_sem.at[f, p]) for p, (mat, cols, own) in enumerate(self.bands(f))]

    def final(self, f):
        rows = ds8(self.core * self.half, self.half)
        moves = [(self.acc.at[f, :, own], self.outs[mat].at[rows, cols]) for mat, cols, own in self.bands(f)]
        far = [remote(src, dst, self.fin_send.at[f, p], self.fin_recv.at[f, p], self.peer) for p, (src, dst) in enumerate(moves)]
        near = [pltpu.make_async_copy(src, dst, self.fin_loc.at[f, p]) for p, (src, dst) in enumerate(moves)]
        return far, near

    def open(self, sub):
        for f in self.flows(sub):
            for copy in self.core_sends(f) + self.core_loads(f):
                copy.start()

    def part(self, step, buf, bit):
        if step < N_RED - 1:
            size = self.half >> (step + 1)
            return buf.at[ds8(bit * size, size), :]
        return buf.at[:, ds_of(bit * (self.lanes // 2), self.lanes // 2, LANE)]

    def ici(self, f, step):
        dev, bit = self.gen(f, step)
        src = self.bufs[step].at[f]
        if step < N_RED:
            src = self.part(step, src, 1 - bit)
        return remote(src, self.bufs[step + 1].at[f], self.ici_send.at[f, step], self.ici_recv.at[f, step], dev)

    def region(self, f, step):
        bits = [self.gen(f, s)[1] for s in range(N_RED)]
        top = min(step, N_RED - 2)
        rows = ds8(sum([bits[s] * (self.half >> (s + 1)) for s in range(top + 1)]), self.half >> (top + 1))
        if step < N_RED - 1:
            return self.acc.at[f, rows, :]
        return self.acc.at[f, rows, ds_of(bits[step] * (self.lanes // 2), self.lanes // 2, LANE)]

    def ag(self, f, step):
        view = self.region(f, step)
        return remote(view, view, self.ag_send.at[f, step], self.ag_recv.at[f, step], self.gen(f, step)[0])

    def reduce(self, step, sub):
        pending = None
        for f in self.flows(sub):
            if step == 0:
                for copy in self.core_loads(f):
                    copy.wait()
                for copy in self.core_sends(f):
                    copy.wait_recv()
                old = self.acc.at[f]
            else:
                self.ici(f, step - 1).wait_recv()
                old = self.bufs[step - 1].at[f]
                if step <= N_RED:
                    old = self.part(step - 1, old, self.gen(f, step - 1)[1])
            cur = self.bufs[step].at[f]
            add_rows(cur, old)
            if step < N_ICI:
                copy = self.ici(f, step)
            else:
                view = self.region(f, N_RED - 1)
                view[...] = cur[...]
                copy = self.ag(f, N_RED - 1)
            if pending is not None:
                pending.start()
            pending = copy
        pending.start()

    def grow(self, step, sub):
        for f in self.flows(sub):
            self.ag(f, step + 1).wait_recv()
            self.ag(f, step).start()

    def finish(self, sub):
        for f in self.flows(sub):
            self.ag(f, 0).wait_recv()
            far, near = self.final(f)
            for copy in far + near:
                copy.start()

    def serve(self, stage, sub):
        if stage == 0:
            self.open(sub)
        elif stage < N_ICI + 2:
            self.reduce(stage - 1, sub)
        elif stage < N_ICI + 4:
            self.grow(N_ICI + 3 - stage, sub)
        else:
            self.finish(sub)

    def close(self):
        for f in range(self.n_flow):
            for copy in self.core_sends(f):
                copy.wait_send()
            for step in range(N_ICI):
                self.ici(f, step).wait_send()
            for step in range(N_RED):
                self.ag(f, step).wait_send()
            far, near = self.final(f)
            for copy in far + near:
                copy.wait()


def comm_scratch(n_sub, srcs):
    rows, width = srcs[0].shape
    n = N_ICI * n_sub
    half, lanes = rows // 2, len(srcs) * width // n
    shapes = [(half, lanes), (half // 2, lanes), (half // 4, lanes)] + [(half // 4, lanes // 2)] * 4
    pieces = 3 - n_sub
    dma = pltpu.SemaphoreType.DMA
    return [pltpu.VMEM((n, half, lanes), F32)] + [pltpu.VMEM((n,) + shape, F32) for shape in shapes] + [dma((n, pieces))] * 3 + [dma((n, N_ICI))] * 2 + [dma((n, N_RED))] * 2 + [dma((n, pieces))] * 3


def all_reduce_kernel(n_mat, *refs):
    srcs, gain_low, gain_top = refs[:n_mat], refs[n_mat], refs[n_mat + 1]
    refs = refs[n_mat + 2:]
    outs, out_g = refs[:n_mat], refs[n_mat]
    gain_src, gain_bufs, g_send, g_recv, g_loc = refs[-5:]
    comm = Comm(SUM_SUB, srcs, outs, refs[n_mat + 1:])

    def gain_copy(step):
        src = gain_src if step == 0 else gain_bufs.at[step - 1]
        dev = comm.peer if step == 0 else comm.gens[step - 1][0]
        return remote(src, gain_bufs.at[step], g_send.at[step], g_recv.at[step], dev)

    gain_src[...] = gain_low[...]
    gain_src[2:4, :] = gain_top[0:2, :]
    comm.barrier()
    for sub in range(SUM_SUB):
        comm.open(sub)
    gain_copy(0).start()
    for step in range(N_ICI + 1):
        for sub in range(SUM_SUB):
            comm.reduce(step, sub)
        gain_copy(step).wait()
        gain_old = gain_src if step == 0 else gain_bufs.at[step - 1]
        gain_bufs[step, :, :] = gain_bufs[step, :, :] + gain_old[...]
        if step < N_ICI:
            gain_copy(step + 1).start()
    gain_out = pltpu.make_async_copy(gain_bufs.at[N_ICI], out_g, g_loc)
    gain_out.start()
    for step in (1, 0):
        for sub in range(SUM_SUB):
            comm.grow(step, sub)
    for sub in range(SUM_SUB):
        comm.finish(sub)
    gain_out.wait()
    comm.close()


def all_reduce(grads, gain_low, gain_top):
    hbm = pl.BlockSpec(memory_space=pl.ANY)
    vmem = pl.BlockSpec(memory_space=pltpu.VMEM)
    dma = pltpu.SemaphoreType.DMA
    n_mat = len(grads)
    return pl.pallas_call(
        functools.partial(all_reduce_kernel, n_mat),
        in_specs=[hbm] * n_mat + [vmem] * 2,
        out_specs=[hbm] * (n_mat + 1),
        out_shape=[jax.ShapeDtypeStruct(grad.shape, F32) for grad in grads] + [jax.ShapeDtypeStruct(gain_low.shape, F32)],
        scratch_shapes=comm_scratch(SUM_SUB, grads) + [pltpu.VMEM(gain_low.shape, F32), pltpu.VMEM((N_ICI + 1,) + gain_low.shape, F32), dma((N_ICI + 1,)), dma((N_ICI + 1,)), dma],
        compiler_params=pltpu.CompilerParams(vmem_limit_bytes=VMEM_PART, collective_id=1, has_side_effects=True),
        name="all_reduce",
    )(*grads, gain_low, gain_top)


def assemble_kernel(n_group, *refs):
    low, top, (sum_g, dx_in), outs = refs[:4], refs[4:8], refs[8:10], refs[10:17]
    grad_ga, grad_gf, dx_out, turned = refs[17:]
    layer, i = pl.program_id(0), pl.program_id(1)
    rows, head_dim = outs[3].shape[0], outs[4].shape[0]
    base = i * (n_group + 2) * head_dim

    def fill(mats):
        for src, dst in zip(mats[:3], outs):
            dst[...] = src[...]

        @pl.when(i == 0)
        def _():
            turned[...] = mats[-1][...].T

    @pl.when(layer == 0)
    def _():
        fill(low)
        dx_out[...] = dx_in[...]
        for row in range(2):
            grad_ga[row:row + 1, :] = sum_g[2 * row:2 * row + 1, :]
            grad_gf[row:row + 1, :] = sum_g[2 * row + 1:2 * row + 2, :]

    @pl.when(layer == 1)
    def _():
        fill(top)

    spots = (base, base + rows, base + rows + head_dim, (pl.num_programs(1) * (n_group + 2) + i * n_group) * head_dim)
    for spot, dst in zip(spots, outs[3:]):
        dst[...] = turned[ds_of(spot, dst.shape[0], head_dim), :]


def assemble(low, top, sum_g, d_x, n_group, head_dim):
    model_dim, ff_dim = low[0].shape
    heads = model_dim // head_dim
    kv_heads = heads // n_group
    rows = n_group * head_dim

    def maps(layer):
        def at(l, i):
            return i * (1 - l) + (kv_heads - 1) * l if layer == 0 else i * l
        return [pl.BlockSpec((rows, ff_dim), lambda l, i: (at(l, i), 0))] * 3 + [pl.BlockSpec(low[3].shape, lambda l, i: (0, 0), pipeline_mode=pl.Buffered(1))]

    out_big = pl.BlockSpec((None, rows, ff_dim), lambda l, i: (l, i, 0))
    out_small = pl.BlockSpec((None, rows, model_dim), lambda l, i: (l, i, 0))
    out_kv = pl.BlockSpec((None, head_dim, model_dim), lambda l, i: (l, i, 0))
    shape = jax.ShapeDtypeStruct
    gain_shape = shape((2, model_dim), F32)
    dx_spec = pl.BlockSpec((rows, d_x.shape[1]), lambda l, i: (i * (1 - l) + (kv_heads - 1) * l, 0))
    big_shape, q_shape, kv_shape = shape((2, model_dim, ff_dim), F32), shape((2, model_dim, model_dim), F32), shape((2, kv_heads * head_dim, model_dim), F32)
    return pl.pallas_call(
        functools.partial(assemble_kernel, n_group),
        grid=(2, kv_heads),
        in_specs=maps(0) + maps(1) + [whole_once(sum_g.shape), dx_spec],
        out_specs=[out_big] * 3 + [out_small, out_kv, out_kv, out_small, whole_once(gain_shape.shape), whole_once(gain_shape.shape), dx_spec],
        out_shape=[big_shape] * 3 + [q_shape, kv_shape, kv_shape, q_shape, gain_shape, gain_shape, shape(d_x.shape, d_x.dtype)],
        scratch_shapes=[pltpu.VMEM(low[3].shape[::-1], F32)],
        compiler_params=pltpu.CompilerParams(vmem_limit_bytes=VMEM_PART),
        name="assemble",
    )(*low, *top, sum_g, d_x)


def whole_once(shape):
    return pl.BlockSpec(shape, lambda *_: (0,) * len(shape), pipeline_mode=pl.Buffered(1))


def qkv_step(x_ref, gain_ref, w_ref, qkv):
    gain = gain_ref[...]

    @pl.loop(0, x_ref.shape[1] // BLK)
    def _(j):
        cols = ds_of(j * BLK, BLK, BLK)
        x_f = x_ref[:, cols].astype(F32)
        inv = lax.rsqrt(jnp.mean(x_f * x_f, axis=0, keepdims=True) + NORM_EPS)
        qkv[:, cols] = dot_nn(w_ref[...], (x_f * inv * gain).astype(BF16)).astype(BF16)


def attn_fwd_step(att_scale, first, q_ref, k_ref, v_ref, cos_ref, sin_ref, a_ref, qr_ref, kr_ref, st_ref, k_scr):
    n_blk = q_ref.shape[1] // BLK
    cos_t = cos_ref[...]
    sin_t = sin_ref[...]

    @pl.when(first)
    def _():
        k_f = k_ref[...].astype(F32)
        k_rot = (k_f * cos_t + pair_swap(k_f) * sin_t).astype(BF16)
        kr_ref[...] = k_rot
        k_scr[...] = k_rot.astype(F32).T.astype(BF16)

    coef = att_scale * LOG2E
    mask = diag_mask()
    q_f = q_ref[...].astype(F32)
    qr_ref[...] = (q_f * cos_t + pair_swap(q_f) * sin_t).astype(BF16)
    for j in range(n_blk):
        cols = slice(j * BLK, (j + 1) * BLK)
        q_j = qr_ref[:, cols]
        s_blocks = []
        for i in range(j + 1):
            s_i = dot_nn(k_scr[i * BLK:(i + 1) * BLK, :], q_j)
            if i == j:
                s_i = jnp.where(mask, s_i, -1e30)
            s_blocks.append(s_i)
        top = functools.reduce(jnp.maximum, [jnp.max(s_i, axis=0, keepdims=True) for s_i in s_blocks])
        e_blocks = [jnp.exp2((s_i - top) * coef) for s_i in s_blocks]
        total = functools.reduce(jnp.add, [jnp.sum(e_i, axis=0, keepdims=True) for e_i in e_blocks])
        inv = 1.0 / total
        acc = None
        for i in range(j + 1):
            p_i = (e_blocks[i] * inv).astype(BF16)
            part = dot_nn(v_ref[:, i * BLK:(i + 1) * BLK], p_i)
            acc = part if acc is None else acc + part
        a_ref[:, cols] = acc.astype(BF16)
        st_ref[0:1, cols] = top
        st_ref[1:2, cols] = inv


def clear(*targets):
    for ref in targets:
        ref[...] = jnp.zeros_like(ref)


def attn_bwd_step(att_scale, first, last, qr_ref, kr_ref, v_ref, do_ref, st_ref, cos_ref, sin_ref, dq_ref, dk_ref, dv_ref, k_scr, v_scr, dk_acc, dv_acc):
    n_blk = qr_ref.shape[1] // BLK

    @pl.when(first)
    def _():
        k_scr[...] = kr_ref[...].astype(F32).T.astype(BF16)
        v_scr[...] = v_ref[...].astype(F32).T.astype(BF16)
        clear(dk_acc)
        clear(dv_acc)

    coef = att_scale * LOG2E
    mask = diag_mask()
    for j in range(n_blk):
        cols = slice(j * BLK, (j + 1) * BLK)
        q_j = qr_ref[:, cols]
        do_j = do_ref[:, cols]
        top = st_ref[0:1, cols]
        inv = st_ref[1:2, cols]
        p_blocks = []
        dp_blocks = []
        row_dot = None
        for i in range(j + 1):
            keys = slice(i * BLK, (i + 1) * BLK)
            s_i = dot_nn(k_scr[keys, :], q_j)
            if i == j:
                s_i = jnp.where(mask, s_i, -1e30)
            p_i = jnp.exp2((s_i - top) * coef) * inv
            dp_i = dot_nn(v_scr[keys, :], do_j).astype(BF16).astype(F32)
            part = jnp.sum(p_i * dp_i, axis=0, keepdims=True)
            row_dot = part if row_dot is None else row_dot + part
            dv_acc[:, keys] += dot_nt(do_j, p_i.astype(BF16))
            p_blocks.append(p_i)
            dp_blocks.append(dp_i)
        dq_j = None
        for i in range(j + 1):
            keys = slice(i * BLK, (i + 1) * BLK)
            ds_i = (p_blocks[i] * (dp_blocks[i] - row_dot) * att_scale).astype(BF16)
            part = dot_nn(kr_ref[:, keys], ds_i)
            dq_j = part if dq_j is None else dq_j + part
            dk_acc[:, keys] += dot_nt(q_j, ds_i)
        dq_j = dq_j.astype(BF16).astype(F32)
        dq_ref[:, cols] = (dq_j * cos_ref[:, cols] - pair_swap(dq_j) * sin_ref[:, cols]).astype(BF16)

    @pl.when(last)
    def _():
        d_k = dk_acc[...].astype(BF16).astype(F32)
        dk_ref[...] = (d_k * cos_ref[...] - pair_swap(d_k) * sin_ref[...]).astype(BF16)
        dv_ref[...] = dv_acc[...].astype(BF16)


def input_step(scale, x_ref, dmid_ref, gain_ref, w_ref, dqkv, dx_ref, gw_ref, gg_ref, w_t, n_scr, gacc):
    clear(gacc)
    gain = gain_ref[...]
    w_t[...] = w_ref[...].T

    @pl.loop(0, x_ref.shape[1] // BLK)
    def _(j):
        cols = ds_of(j * BLK, BLK, BLK)
        x_f = x_ref[:, cols].astype(F32)
        inv = lax.rsqrt(jnp.mean(x_f * x_f, axis=0, keepdims=True) + NORM_EPS)
        n_scr[:, cols] = (x_f * inv * gain).astype(BF16)
        d_normed = dot_nn(w_t[...], dqkv[:, cols]).astype(BF16).astype(F32)
        d_resid, d_gain = norm_back_cols(x_f, inv, gain, d_normed)
        gacc[...] += fold_lanes(d_gain)
        dx_ref[:, cols] = (dmid_ref[:, cols].astype(F32) + d_resid).astype(BF16)

    gw_ref[...] = dot_nt(n_scr[...], dqkv[...]) * scale
    gg_ref[...] = jnp.sum(gacc[...].T, axis=0, keepdims=True) * scale


def ffn_step(scale, first, last, x_ref, a_ref, dout_ref, wo_ref, gain_ref, wg_ref, wu_ref, wd_ref, gwo_ref, gg_ref, gwg_ref, gwu_ref, gwd_ref, m_scr, n_scr, inv_scr, acc, hid, dg, du, wg_t, wu_t, wd_t, wo_t, gacc):
    n_blk = x_ref.shape[1] // BLK
    gain = gain_ref[...]

    @pl.when(first)
    def _():
        wo_t[...] = wo_ref[...].T

        @pl.loop(0, n_blk)
        def _(j):
            cols = ds_of(j * BLK, BLK, BLK)
            m_b = (x_ref[:, cols].astype(F32) + dot_nn(wo_t[...], a_ref[:, cols])).astype(BF16)
            m_scr[:, cols] = m_b
            m_f = m_b.astype(F32)
            inv = lax.rsqrt(jnp.mean(m_f * m_f, axis=0, keepdims=True) + NORM_EPS)
            inv_scr[0:1, cols] = inv
            n_scr[:, cols] = (m_f * inv * gain).astype(BF16)
        clear(acc)
        clear(gacc)

    wg_t[...] = wg_ref[...].T
    wu_t[...] = wu_ref[...].T
    wd_t[...] = wd_ref[...].T
    for j in range(n_blk):
        cols = slice(j * BLK, (j + 1) * BLK)
        gate_f = dot_nn(wg_t[...], n_scr[:, cols]).astype(BF16).astype(F32)
        up_f = dot_nn(wu_t[...], n_scr[:, cols]).astype(BF16).astype(F32)
        d_hidden = dot_nn(wd_t[...], dout_ref[:, cols]).astype(BF16).astype(F32)
        gate_sig = jax.nn.sigmoid(gate_f)
        silu_act = gate_f * gate_sig
        hid[:, cols] = (silu_act * up_f).astype(BF16)
        dg[:, cols] = (d_hidden * up_f * gate_sig * (1.0 + gate_f * (1.0 - gate_sig))).astype(BF16)
        du[:, cols] = (d_hidden * silu_act).astype(BF16)
        acc[:, cols] += dot_nn(wg_ref[...], dg[:, cols]) + dot_nn(wu_ref[...], du[:, cols])
    gwg_ref[...] = dot_nt(n_scr[...], dg[...]) * scale
    gwu_ref[...] = dot_nt(n_scr[...], du[...]) * scale
    gwd_ref[...] = dot_nt(dout_ref[...], hid[...]) * scale

    @pl.when(last)
    def _():

        @pl.loop(0, n_blk)
        def _(j):
            cols = ds_of(j * BLK, BLK, BLK)
            d_normed = acc[:, cols].astype(BF16).astype(F32)
            d_resid, d_gain = norm_back_cols(m_scr[:, cols].astype(F32), inv_scr[0:1, cols], gain, d_normed)
            gacc[...] += fold_lanes(d_gain)
            d_mid = (dout_ref[:, cols].astype(F32) + d_resid).astype(BF16)
            m_scr[:, cols] = d_mid

        gwo_ref[...] = dot_nt(m_scr[...], a_ref[...]) * scale
        a_ref[...] = dot_nn(wo_ref[...], m_scr[...]).astype(BF16)
        gg_ref[...] = jnp.sum(gacc[...].T, axis=0, keepdims=True) * scale


COMM_AT = ((0, 2, 7, 10, 11, 12, 13, 14, 15, 17, 20), (0, 5, 9, 11, 12, 13, 14, 15, 16, 19, 22))


def layer_kernel(layer, scale, dims, pl_steps, n_src, *refs):
    kv_heads, n_group, head_dim = dims
    refs = list(refs)
    x_ref, dout_ref, wq_ref, wk_ref, wv_ref, wo_ref, ga_in, gf_in, cos_ref, sin_ref, wg_ref, wu_ref, wd_ref = refs[:13]
    srcs = refs[13:13 + n_src]
    pos = 13 + n_src
    dx_ref, gb_ref, gains_ref, gwg_ref, gwu_ref, gwd_ref = refs[pos:pos + 6]
    outs = refs[pos + 6:pos + 6 + n_src]
    pos = pos + 6 + n_src
    qkv, a_scr, qr, kr, st, k_scr, v_scr, dk_acc, dv_acc, m_scr, n_scr, inv_scr, acc, hid, dg, du, wg_t, wu_t, wd_t, wo_t, wqkv_t, gacc, wqkv_ref, ga_ref, gf_ref = refs[pos:pos + 25]
    comm_refs = refs[pos + 25:]
    step = pl.program_id(0)
    heads = kv_heads * n_group
    n_ffn = pl.num_programs(0) - 2 * heads
    att_scale = head_dim ** -0.5
    per = (n_group + 2) * head_dim

    if n_src:
        comm = Comm(LAYER_SUB, srcs, outs, comm_refs)
        for at in range(pl_steps):
            todo = [(stage, sub) for stage in range(len(COMM_AT[0])) for sub in range(LAYER_SUB) if COMM_AT[sub][stage] == at]
            if todo:
                @pl.when(step == at)
                def _(todo=todo, at=at):
                    if at == 0:
                        comm.barrier()
                    for stage, sub in todo:
                        comm.serve(stage, sub)

    @pl.when(step == 0)
    def _():
        q_rows = n_group * head_dim
        for g in range(kv_heads):
            wqkv_ref[g * per:g * per + q_rows, :] = wq_ref[g * q_rows:(g + 1) * q_rows, :]
            wqkv_ref[g * per + q_rows:g * per + q_rows + head_dim, :] = wk_ref[g * head_dim:(g + 1) * head_dim, :]
            wqkv_ref[g * per + q_rows + head_dim:(g + 1) * per, :] = wv_ref[g * head_dim:(g + 1) * head_dim, :]
        for src, dst in ((ga_in, ga_ref), (gf_in, gf_ref)):
            row = src[...].astype(F32)[layer:layer + 1, :]
            dst[...] = jnp.broadcast_to(row, (8, row.shape[1])).T[:, 0:1]
        clear(gains_ref)
        qkv_step(x_ref, ga_ref, wqkv_ref, qkv)

    def head_views(idx):
        g, h = idx // n_group, lax.rem(idx, n_group)
        base = g * per
        rows_q = ds_of(base + h * head_dim, head_dim, head_dim)
        rows_k = ds_of(base + n_group * head_dim, head_dim, head_dim)
        rows_v = ds_of(base + (n_group + 1) * head_dim, head_dim, head_dim)
        return h, qkv.at[rows_q, :], qkv.at[rows_k, :], qkv.at[rows_v, :], a_scr.at[ds_of(idx * head_dim, head_dim, head_dim), :], qr.at[ds_of(idx * head_dim, head_dim, head_dim), :], kr.at[ds_of(g * head_dim, head_dim, head_dim), :], st.at[idx]

    @pl.when(step < heads)
    def _():
        h, q_v, k_v, v_v, a_v, qr_v, kr_v, st_v = head_views(step)
        attn_fwd_step(att_scale, h == 0, q_v, k_v, v_v, cos_ref, sin_ref, a_v, qr_v, kr_v, st_v, k_scr)

    @pl.when((step >= heads) & (step < heads + n_ffn))
    def _():
        ffn_step(scale, step == heads, step == heads + n_ffn - 1, x_ref, a_scr, dout_ref, wo_ref, gf_ref, wg_ref, wu_ref, wd_ref, gb_ref.at[:, per * kv_heads:], gains_ref.at[1:2, :], gwg_ref, gwu_ref, gwd_ref, m_scr, n_scr, inv_scr, acc, hid, dg, du, wg_t, wu_t, wd_t, wo_t, gacc)

    @pl.when(step >= heads + n_ffn)
    def _():
        h, q_v, k_v, v_v, a_v, qr_v, kr_v, st_v = head_views(step - heads - n_ffn)
        attn_bwd_step(att_scale, h == 0, h == n_group - 1, qr_v, kr_v, v_v, a_v, st_v, cos_ref, sin_ref, q_v, k_v, v_v, k_scr, v_scr, dk_acc, dv_acc)

    @pl.when(step == pl.num_programs(0) - 1)
    def _():
        input_step(scale, x_ref, m_scr, ga_ref, wqkv_ref, qkv, dx_ref, gb_ref.at[:, :per * kv_heads], gains_ref.at[0:1, :], wqkv_t, n_scr, gacc)
        if n_src:
            comm.close()


def layer_call(layer, x_t, d_out_t, weights, cos_t, sin_t, scale, dims, other=None):
    g_attn, wq_t, wk_t, wv_t, w_o, g_ffn, w_gate, w_up, wd_t = weights
    kv_heads, n_group, head_dim = dims
    model_dim, seq_len = x_t.shape
    ff_dim = w_gate.shape[2]
    heads = kv_heads * n_group
    n_ffn = ff_dim // BLK
    qkv_rows = (heads + 2 * kv_heads) * head_dim
    w_spec = pl.BlockSpec((None, model_dim, BLK), lambda t: (layer, 0, jnp.minimum(jnp.maximum(t - heads, 0), n_ffn - 1)))
    g_spec = pl.BlockSpec((model_dim, BLK), lambda t: (0, jnp.minimum(jnp.maximum(t - heads, 0), n_ffn - 1)))
    hbm = pl.BlockSpec(memory_space=pl.ANY)

    def one(w):
        return pl.BlockSpec((None,) + w.shape[1:], lambda t: (layer, 0, 0), pipeline_mode=pl.Buffered(1))

    in_specs = [whole_once(x_t.shape), whole_once(x_t.shape), one(wq_t), one(wk_t), one(wv_t), one(w_o), whole_once(g_attn.shape), whole_once(g_ffn.shape), whole_once(cos_t.shape), whole_once(cos_t.shape), w_spec, w_spec, w_spec]
    args = [x_t, d_out_t, wq_t, wk_t, wv_t, w_o, g_attn, g_ffn, cos_t, sin_t, w_gate, w_up, wd_t]
    shape = jax.ShapeDtypeStruct
    qkv_w, o_w, grad_w, gain_w = (qkv_rows, model_dim), w_o.shape[1:], w_gate.shape[1:], (8, model_dim)
    out_specs = [whole_once(x_t.shape), whole_once(grad_w), whole_once(gain_w), g_spec, g_spec, g_spec]
    out_shape = [shape(x_t.shape, BF16), shape(grad_w, F32), shape(gain_w, F32)] + [shape(grad_w, F32)] * 3
    vm = pltpu.VMEM
    tok = (seq_len, head_dim)
    scratch = [vm((qkv_rows, seq_len), BF16), vm((heads * head_dim, seq_len), BF16), vm((heads * head_dim, seq_len), BF16), vm((kv_heads * head_dim, seq_len), BF16), vm((heads, 8, seq_len), F32)]
    scratch += [vm(tok, BF16), vm(tok, BF16), vm(tok[::-1], F32), vm(tok[::-1], F32), vm(x_t.shape, BF16), vm(x_t.shape, BF16), vm((8, seq_len), F32), vm(x_t.shape, F32)]
    scratch += [vm((BLK, seq_len), BF16)] * 3 + [vm((BLK, model_dim), BF16)] * 3 + [vm(o_w[::-1], BF16), vm(qkv_w[::-1], BF16), vm((model_dim, 128), F32), vm(qkv_w, BF16), vm((model_dim, 1), F32), vm((model_dim, 1), F32)]
    n_src = 0
    params = {}
    if other is not None:
        n_src = len(other)
        args += list(other)
        in_specs += [hbm] * n_src
        out_specs += [hbm] * n_src
        out_shape += [shape(grad.shape, F32) for grad in other]
        scratch += comm_scratch(LAYER_SUB, other)
        params = dict(collective_id=0, has_side_effects=True)
    return pl.pallas_call(
        functools.partial(layer_kernel, layer, scale, dims, 2 * heads + n_ffn, n_src),
        grid=(2 * heads + n_ffn,),
        in_specs=in_specs,
        out_specs=out_specs,
        out_shape=out_shape,
        scratch_shapes=scratch,
        compiler_params=pltpu.CompilerParams(vmem_limit_bytes=VMEM_ALL, **params),
        cost_estimate=pl.CostEstimate(flops=24 * x_t.size * ff_dim, bytes_accessed=20 * grad_w[0] * grad_w[1], transcendentals=0),
        name="layer" if other is None else "layer_and_sum",
    )(*args)


def solution(mesh):
    num_devices = mesh.shape["dp"]
    act_spec = P("dp", None, None)
    rep_spec = P()

    def local_step(x_layer0, x_layer1, d_out, g_attn, w_q, w_k, w_v, w_o, g_ffn, w_gate, w_up, w_down):
        _, seq_len, model_dim = x_layer0.shape
        n_heads, head_dim = w_q.shape[2], w_q.shape[3]
        kv_heads = w_k.shape[2]
        n_group = n_heads // kv_heads
        cos_np, sin_np = rope_tables_np(seq_len, head_dim)
        cos_t, sin_t = jnp.asarray(cos_np), jnp.asarray(sin_np)
        scale = 1.0 / num_devices

        def heads_out(w):
            return jnp.transpose(w, (0, 2, 3, 1)).reshape(2, -1, model_dim)

        weights = (g_attn, heads_out(w_q), heads_out(w_k), heads_out(w_v), w_o.reshape(2, -1, model_dim), g_ffn, w_gate, w_up, jnp.transpose(w_down, (0, 2, 1)))
        x0_t = jnp.transpose(x_layer0[0], (1, 0))
        x1_t = jnp.transpose(x_layer1[0], (1, 0))
        d_top = jnp.transpose(d_out[0], (1, 0))
        dims = (kv_heads, n_group, head_dim)
        d_mid, gb1, gains1, gg1, gu1, gd1 = layer_call(1, x1_t, d_top, weights, cos_t, sin_t, scale, dims)
        low = layer_call(0, x0_t, d_mid, weights, cos_t, sin_t, scale, dims, (gg1, gu1, gd1, gb1))
        d_x0, gb0, gains0, gg0, gu0, gd0 = low[:6]
        sums = all_reduce((gg0, gu0, gd0, gb0), gains0, gains1)
        sum_g = sums[4]
        sum_gate, sum_up, sum_wd, sum_q, sum_k, sum_v, sum_o, grad_ga, grad_gf, d_x0 = assemble(sums[:4], low[6:], sum_g, d_x0, n_group, head_dim)

        def heads_in(g):
            return jnp.transpose(g.reshape(2, -1, head_dim, model_dim), (0, 3, 1, 2))

        d_x = jnp.transpose(d_x0, (1, 0))[None]
        return (d_x, grad_ga, heads_in(sum_q), heads_in(sum_k), heads_in(sum_v), sum_o.reshape(2, n_heads, head_dim, model_dim), grad_gf, sum_gate, sum_up, jnp.transpose(sum_wd, (0, 2, 1)))

    return jax.shard_map(local_step, mesh=mesh, in_specs=(act_spec, act_spec, act_spec) + (rep_spec,) * 9, out_specs=(act_spec,) + (rep_spec,) * 9, check_vma=False)
```
